512 devices in a mesh: cube: 2 (over y), gz: 128 (over x, z), gy: 2 (over core).
Axes of the slice: x: 8, y: 2, z: 16, core: 2. Of those that a mesh axis runs over, the one named last changes fastest.
The devices are a block of a 8x8x16 slice.
Arguments:
- noisy_cube: float32 [1024, 64, 256], P(('cube', 'gz'), 'gy'), parts along dimension 0, may hold values from -40 to 40
- thresholds: float32 [4], replicated, may hold values from 0.5 to 4
Outputs:
- denoised: float32 [1024, 4, 64, 256], P(('cube', 'gz'), None, 'gy'), parts along dimension 0
- gcv_score: float32 [8], P('cube'), parts along dimension 0
The draws below stay inside these ranges and needn't reach their ends.
There are 2 independent parts, one for each index of `cube`. The reference program is written for one: setup_inputs(seed, part) draws one part's arguments, and reference() takes and returns one part's arrays. A program takes and returns all parts, laid end to end along the dimension named above; an argument that names none is the same for every part. Nothing has to cross between parts.
All inputs are finite; a program needn't handle non-finite values.
Results may differ from the reference program's by a relative error of at most 0.0003.
Values sent between devices are 32-bit elements; how exact they have to be, the bound alone decides.
A program may use at most 64 MiB of HBM per device.

```python
import math
import jax
import jax.numpy as jnp
from jax import lax

NX = 256
NT = 4
NZ = 512
NY = 64


def draw_noisy_cube(key, part):
    subkeys = jax.random.split(jax.random.fold_in(key, 17), 2)
    phases = jax.random.uniform(subkeys[0], (3,), jnp.float32, -math.pi, math.pi)
    z_frac = jnp.arange(NZ, dtype=jnp.float32) / NZ
    y_frac = jnp.arange(NY, dtype=jnp.float32) / NY
    x_frac = jnp.arange(NX, dtype=jnp.float32) / NX
    signal = 2.0 * jnp.sin(2.0 * math.pi * 3.0 * z_frac + phases[0])[:, None, None]
    signal = signal * jnp.cos(2.0 * math.pi * 2.0 * y_frac + phases[1])[None, :, None]
    signal = signal * jnp.sin(2.0 * math.pi * 5.0 * x_frac + phases[2])[None, None, :]
    z_rise = 3.0 ** (jnp.arange(NZ, dtype=jnp.float32) / (NZ - 1))
    y_rise = 3.0 ** (jnp.arange(NY, dtype=jnp.float32) / (NY - 1))
    scaling = z_rise[:, None, None] * y_rise[None, :, None]
    jitter = jax.random.truncated_normal(subkeys[1], -4.0, 4.0, (NZ, NY, NX), jnp.float32)
    return signal + scaling * jitter


def setup_inputs(seed: int = 0, part: int = 0) -> dict:
    arg_keys = jax.random.split(jax.random.key(seed), 3)
    part_keys = jax.random.split(jax.random.fold_in(arg_keys[2], part), 3)
    return {
        "noisy_cube": draw_noisy_cube(jax.random.fold_in(jax.random.fold_in(arg_keys[2], part), 71), part),
        "thresholds": jnp.clip(jnp.exp(jax.random.uniform(arg_keys[1], (NT,), jnp.float32, math.log(0.5), math.log(4.0))), 0.5, 4.0),
    }


LOWPASS = (0.2303778133088964, 0.7148465705529154, 0.6308807679298587, -0.0279837694168599,
           -0.1870348117190931, 0.0308413818355607, 0.0328830116668852, -0.0105974017850690)
HIGHPASS = tuple(((-1) ** tap_index) * LOWPASS[7 - tap_index] for tap_index in range(8))
lead_taps = 6
trail_taps = 3


def analyse(extended, dimension_number, axis_length):
    lowband = 0.0
    highband = 0.0
    for tap_index in range(8):
        sliced = lax.slice_in_dim(extended, tap_index, tap_index + axis_length - 1, 2, dimension_number)
        lowband = lowband + LOWPASS[tap_index] * sliced
        highband = highband + HIGHPASS[tap_index] * sliced
    return lowband, highband


def synthesise(lowband, highband, dimension_number, axis_length):
    even_part = 0.0
    odd_part = 0.0
    for tap_index in range(4):
        low_slice = lax.slice_in_dim(lowband, 3 - tap_index, 3 - tap_index + axis_length, 1, dimension_number)
        high_slice = lax.slice_in_dim(highband, 3 - tap_index, 3 - tap_index + axis_length, 1, dimension_number)
        even_part = even_part + LOWPASS[2 * tap_index] * low_slice + HIGHPASS[2 * tap_index] * high_slice
        odd_part = odd_part + LOWPASS[2 * tap_index + 1] * low_slice + HIGHPASS[2 * tap_index + 1] * high_slice
    paired = jnp.stack([even_part, odd_part], dimension_number + 1)
    target = list(even_part.shape)
    target[dimension_number] = 2 * axis_length
    return paired.reshape(target)


def merge_bands(lowband, highband):
    stacked = jnp.stack([lowband, highband], 2)
    return stacked.reshape((lowband.shape[0], 2 * lowband.shape[1]) + lowband.shape[2:])


def split_bands(current):
    halves = current.reshape((current.shape[0], current.shape[1] // 2, 2) + current.shape[2:])
    return halves[:, :, 0], halves[:, :, 1]


def wrap_ahead(input_tensor, dimension_number, border_extent):
    return jnp.concatenate([input_tensor, lax.slice_in_dim(input_tensor, 0, border_extent, 1, dimension_number)], dimension_number)


def wrap_behind(input_tensor, dimension_number, border_extent):
    axis_length = input_tensor.shape[dimension_number]
    return jnp.concatenate([lax.slice_in_dim(input_tensor, axis_length - border_extent, axis_length, 1, dimension_number), input_tensor], dimension_number)


def forward_level(volume):
    planes, number_of_lines, col_count = volume.shape[0], volume.shape[2], volume.shape[3]
    lowband, highband = analyse(wrap_ahead(volume, 0, lead_taps), 0, planes)
    banded = merge_bands(lowband, highband)
    lowband, highband = analyse(wrap_ahead(banded, 2, lead_taps), 2, number_of_lines)
    banded = merge_bands(lowband, highband)
    lowband, highband = analyse(wrap_ahead(banded, 3, lead_taps), 3, col_count)
    return merge_bands(lowband, highband)


def synth_x(current):
    lowband, highband = split_bands(current)
    return synthesise(wrap_behind(lowband, 3, trail_taps), wrap_behind(highband, 3, trail_taps), 3, current.shape[3])


def synth_y(extended, number_of_lines):
    lowband, highband = split_bands(extended)
    return synthesise(lowband, highband, 2, number_of_lines)


def synth_z(extended, planes):
    lowband, highband = split_bands(extended)
    return synthesise(lowband, highband, 0, planes)


def inverse_level(coeffs):
    planes, number_of_lines = coeffs.shape[0], coeffs.shape[2]
    current = synth_x(coeffs)
    current = synth_y(wrap_behind(current, 2, trail_taps), number_of_lines)
    return synth_z(wrap_behind(current, 0, trail_taps), planes)


def spread(details, approximation, limits):
    bounds = limits[None, :, None, None, None]
    widened = details[:, None]
    shrunk = widened - jnp.clip(widened, -bounds, bounds)
    complete = jnp.concatenate([approximation[:, :, None], shrunk], 2)
    return complete.reshape((complete.shape[0], complete.shape[1] * 8) + complete.shape[3:])


def reference(noisy_cube, thresholds):
    level_one = forward_level(noisy_cube[:, None])
    level_two = forward_level(level_one[:, :1])
    details_one = level_one[:, 1:]
    details_two = level_two[:, 1:]
    cell_count = NZ * NY * NX

    def single(threshold):
        limits = threshold[None]
        approximation = inverse_level(spread(details_two, level_two[:, :1], limits))
        rebuilt = inverse_level(spread(details_one, approximation, limits))[:, 0]
        residual = jnp.sum((rebuilt - noisy_cube) ** 2)
        square = threshold * threshold
        zero_weight = jnp.sum(square / (square + details_one * details_one)) + jnp.sum(square / (square + details_two * details_two))
        return rebuilt, cell_count * residual / (zero_weight * zero_weight)

    stacked, gcv_score = lax.map(single, thresholds)
    return jnp.transpose(stacked, (1, 0, 2, 3)), gcv_score
```

```python
import functools

import jax
import jax.numpy as jnp
import numpy as np
from jax import lax
from jax.experimental import pallas as pl
from jax.experimental.pallas import tpu as pltpu
from jax.sharding import Mesh
from jax.sharding import PartitionSpec as P

MESH = pl.DeviceIdType.MESH
CUBE_GZ = ("cube", "gz_0", "gz_1")

LOWPASS = (
    0.2303778133088964,
    0.7148465705529155,
    0.6308807679298587,
    -0.0279837694168599,
    -0.1870348117190931,
    0.0308413818355607,
    0.0328830116668852,
    -0.010597401785069,
)
HIGHPASS = tuple(((-1) ** tap * LOWPASS[7 - tap] for tap in range(8)))


def composed(second):
    taps = np.zeros(22)
    for outer in range(8):
        for inner in range(8):
            taps[2 * outer + inner] += second[outer] * LOWPASS[inner]
    return tuple(float(tap) for tap in taps)


DEEP_LOW = composed(LOWPASS)
DEEP_HIGH = composed(HIGHPASS)


def analysis_matrix(length):
    matrix = np.zeros((length, length))
    for k in range(length // 2):
        for tap in range(8):
            matrix[(2 * k + tap) % length, k] += LOWPASS[tap]
            matrix[(2 * k + tap) % length, length // 2 + k] += HIGHPASS[tap]
    return matrix


def in_two_parts(matrix):
    exact = matrix.astype(np.float32)
    upper = exact.astype(jnp.bfloat16)
    lower = (exact - upper.astype(np.float32)).astype(jnp.bfloat16)
    return np.stack([upper, lower])


def product(values, parts):
    upper = values.astype(jnp.bfloat16)
    lower = (values - upper.astype(jnp.float32)).astype(jnp.bfloat16)
    dot = functools.partial(jnp.dot, preferred_element_type=jnp.float32)
    return dot(upper, parts[0]) + (dot(lower, parts[0]) + dot(upper, parts[1]))


def weighted(taps, values):
    result = taps[0] * values[0]
    for tap, value in zip(taps[1:], values[1:]):
        result = result + tap * value
    return result


def synthesis_pair(low, high, odd):
    return weighted(LOWPASS[odd::2], low) + weighted(HIGHPASS[odd::2], high)


def shrunk(values, limit):
    return values - jnp.clip(values, -limit, limit)


def kernel(
    nx,
    nz,
    thr,
    x_hbm,
    a1_hbm,
    a1t_hbm,
    a2_hbm,
    a2t_hbm,
    den,
    gcv,
    raw,
    xa,
    ll,
    l2x,
    zb,
    lz,
    db,
    cb,
    zs2,
    co,
    cr,
    zs1,
    fo,
    a1,
    a1t,
    a2,
    a2t,
    row,
    tot,
    arx,
    arz,
    local_sem,
    send_sem,
    recv_sem,
    near_sem,
    mid_sem,
    far_sem,
):
    cube, gx, gz, gy = (lax.axis_index(n) for n in ("cube", "gz_0", "gz_1", "gy"))
    total = nx * nz
    flat = gx * nz + gz
    other = 1 - gy
    other_core = (cube, gx, gz, other)

    def along(offset):
        place = lax.rem(flat + (offset + total), total)
        return (cube, lax.div(place, nz), lax.rem(place, nz), gy)

    def across_x(offset, core):
        return (cube, lax.rem(gx + (offset + nx), nx), gz, core)

    def across_z(offset):
        return (cube, gx, lax.rem(gz + offset, nz), gy)

    sent = []

    def send(src, dst, device):
        index = len(sent)
        copy = pltpu.make_async_remote_copy(
            src_ref=src,
            dst_ref=dst,
            send_sem=send_sem.at[index],
            recv_sem=recv_sem.at[index],
            device_id=device,
            device_id_type=MESH,
        )
        copy.start()
        sent.append(copy)
        return copy

    def signal(sem, device):
        pl.semaphore_signal(sem, inc=1, device_id=device, device_id_type=MESH)

    loads = [pltpu.make_async_copy(x_hbm, raw.at[:, 0:32, :], local_sem.at[0])]
    for index, (src, dst) in enumerate(
        ((a1_hbm, a1), (a2_hbm, a2), (a2t_hbm, a2t), (a1t_hbm, a1t))
    ):
        loads.append(pltpu.make_async_copy(src, dst, local_sem.at[index + 1]))
    for load in loads:
        load.start()

    barrier = pltpu.get_barrier_semaphore()
    nearest = (along(1), along(-1), across_x(1, gy), across_x(-1, gy))
    for device in (other_core,) + nearest:
        signal(barrier, device)
    pl.semaphore_wait(barrier, 5)

    loads[0].wait()
    rows_copy = send(raw.at[:, 0:24, :], raw.at[:, 32:56, :], other_core)

    for device in nearest:
        signal(near_sem, device)
    pl.semaphore_wait(near_sem, 4)
    for device in (along(2), along(-2), across_x(2, gy), across_x(-2, gy)):
        signal(mid_sem, device)

    loads[1].wait()
    own = product(raw[:, 0:32, :].reshape(128, 256), a1)
    for sx in range(2):
        xa[sx, :, 0:32, :] = own[:, 128 * sx : 128 * sx + 128].reshape(4, 32, 128)
    rows_copy.wait_recv()
    beyond = product(raw[:, 32:56, :].reshape(96, 256), a1)
    for sx in range(2):
        xa[sx, :, 32:56, :] = beyond[:, 128 * sx : 128 * sx + 128].reshape(4, 24, 128)

    for z in range(4):
        for sx in range(2):
            taps = [xa[sx, z, pl.ds(j, 16, stride=2), :] for j in range(8)]
            low = weighted(LOWPASS, taps)
            zb[4 + z, sx] = low
            zb[4 + z, 2 + sx] = weighted(HIGHPASS, taps)
            if sx == 0:
                ll[z, 0:16, :] = low
                taps = [xa[sx, z, pl.ds(32 + j, 8, stride=2), :] for j in range(8)]
                ll[z, 16:24, :] = weighted(LOWPASS, taps)

    loads[2].wait()
    l2x[...] = product(ll[...].reshape(96, 128), a2).reshape(4, 24, 128)
    for z in range(4):
        taps = [l2x[z, pl.ds(j, 8, stride=2), :] for j in range(8)]
        lz[8 + z, 0] = weighted(LOWPASS, taps)
        lz[8 + z, 1] = weighted(HIGHPASS, taps)

    deep = lz.at[8:12]
    deep_copies = [
        send(deep, lz.at[0:4], along(2)),
        send(deep, lz.at[16:20], along(-2)),
        send(deep, lz.at[4:8], along(1)),
        send(deep, lz.at[12:16], along(-1)),
    ]
    pl.semaphore_wait(mid_sem, 4)
    deep_copies.append(send(lz.at[8:10], lz.at[20:22], along(-3)))
    for device in (along(4), along(-4), other_core):
        signal(far_sem, device)
    plane_copies = [
        send(zb.at[4:8], zb.at[0:4], along(1)),
        send(zb.at[4:6], zb.at[8:10], along(-1)),
    ]

    limits = [thr[t] for t in range(4)]
    squares = [limit * limit for limit in limits]
    lane = lax.broadcasted_iota(jnp.int32, (8, 128), 1)
    first_half = lane < 64
    zero = jnp.zeros((8, 128), jnp.float32)

    for copy in deep_copies:
        copy.wait_recv()
    for sy in range(2):
        planes = [lz[i, sy] for i in range(22)]
        cb[3, 0, sy, 8:16, :] = weighted(DEEP_LOW, planes)
        cb[3, 1, sy, 8:16, :] = weighted(DEEP_HIGH, planes)
    coeff_copies = [
        send(cb.at[3, :, :, 8:16, :], cb.at[3 - offset, :, :, 8:16, :], along(offset))
        for offset in (3, -2, 2, -1, 1)
    ]

    residual = [zero] * 4
    weight = [zero] * 4
    for sz in range(2):
        for sy in range(2):
            c = cb[3, sz, sy, 8:16, :]
            square = c * c
            for t in range(4):
                cut = jnp.clip(c, -limits[t], limits[t])
                kept = squares[t] / (squares[t] + square)
                cut = cut * cut
                if sz == 0 and sy == 0:
                    cut = jnp.where(first_half, zero, cut)
                    kept = jnp.where(first_half, zero, kept)
                residual[t] = residual[t] + cut
                weight[t] = weight[t] + kept

    for copy in plane_copies:
        copy.wait_recv()
    for band in range(4):
        for k in range(2):
            planes = [zb[2 * k + j, band] for j in range(8)]
            if band:
                db[1 + k, band - 1, 8:24, :] = weighted(LOWPASS, planes)
            db[1 + k, 3 + band, 8:24, :] = weighted(HIGHPASS, planes)
    detail_copies = [
        send(db.at[1:3, :, 8:24, :], db.at[3:5, :, 8:24, :], along(-1)),
        send(db.at[2, :, 8:24, :], db.at[0, :, 8:24, :], along(1)),
    ]

    def add_band(band, sums):
        sums = list(sums)
        for k in range(2):
            for part in range(2):
                c = db[1 + k, band, 8 + 8 * part : 16 + 8 * part, :]
                square = c * c
                for t in range(4):
                    cut = jnp.clip(c, -limits[t], limits[t])
                    sums[t] = sums[t] + cut * cut
                    sums[4 + t] = sums[4 + t] + squares[t] / (squares[t] + square)
        return tuple(sums)

    sums = lax.fori_loop(0, 7, add_band, tuple(residual + weight))

    def as_row(parts):
        line = jnp.zeros((1, 128), jnp.float32)
        for t, part in enumerate(parts):
            value = jnp.sum(jnp.sum(part, axis=0, keepdims=True), axis=1, keepdims=True)
            line = jnp.where(lane[0:1] == t, value, line)
        return line

    row[0:1, :] = as_row(sums[0:4])
    row[1:2, :] = as_row(sums[4:8])
    slot = gy * nx + gx
    arx[pl.ds(slot, 1)] = row[...].reshape(1, 2, 128)
    pl.semaphore_wait(far_sem, 3)
    x_copies = [
        send(row, arx.at[slot], across_x(offset, core))
        for core in (gy, other)
        for offset in range(nx)
        if not (core is gy and offset == 0)
    ]

    for copy in coeff_copies:
        copy.wait_recv()
    deep_rows = send(cb.at[:, :, :, 8:16, :], cb.at[:, :, :, 0:8, :], other_core)
    for copy in detail_copies:
        copy.wait_recv()
    detail_rows = send(db.at[:, :, 16:24, :], db.at[:, :, 0:8, :], other_core)

    for copy in x_copies:
        copy.wait_recv()
    tot[...] = jnp.sum(arx[...], axis=0)
    arz[pl.ds(gz, 1)] = tot[...].reshape(1, 2, 128)
    z_copies = [send(tot, arz.at[gz], across_z(offset)) for offset in range(1, nz)]

    deep_rows.wait_recv()

    def deep_along_z(t, carry):
        limit = thr[t]
        for sy in range(2):
            for part in range(2):
                bands = []
                for sz in range(2):
                    values = []
                    for m in range(6):
                        c = cb[m, sz, sy, 8 * part : 8 * part + 8, :]
                        s = shrunk(c, limit)
                        values.append(jnp.where(first_half, c, s) if sz + sy == 0 else s)
                    bands.append(values)
                for k in range(5):
                    p = 3 + (k + 1) // 2
                    odd = (k + 1) % 2
                    order = [p - i for i in range(4)]
                    zs2[t, k, sy, 8 + 8 * part : 16 + 8 * part, :] = synthesis_pair(
                        [bands[0][i] for i in order], [bands[1][i] for i in order], odd
                    )
        return carry

    lax.fori_loop(0, 4, deep_along_z, 0)

    def deep_along_y(t, carry):
        for k in range(5):
            low = [zs2[t, k, 0, 8 - i : 24 - i, :] for i in range(4)]
            high = [zs2[t, k, 1, 8 - i : 24 - i, :] for i in range(4)]
            co[t, k, pl.ds(0, 16, stride=2), :] = synthesis_pair(low, high, 0)
            co[t, k, pl.ds(1, 16, stride=2), :] = synthesis_pair(low, high, 1)
        return carry

    lax.fori_loop(0, 4, deep_along_y, 0)
    loads[3].wait()
    cr[...] = product(co[:, :, 8:32, :].reshape(480, 128), a2t).reshape(4, 5, 24, 128)

    detail_rows.wait_recv()

    def along_z(t, carry):
        limit = thr[t]
        for part in range(3):
            rows = slice(8 * part, 8 * part + 8)
            for band in range(4):
                if band:
                    low = [shrunk(db[k, band - 1, rows, :], limit) for k in range(5)]
                else:
                    low = [cr[t, k, rows, :] for k in range(5)]
                high = [shrunk(db[k, 3 + band, rows, :], limit) for k in range(5)]
                for e in range(2):
                    order = [3 + e - i for i in range(4)]
                    for odd in range(2):
                        zs1[2 * e + odd, t, band, rows, :] = synthesis_pair(
                            [low[i] for i in order], [high[i] for i in order], odd
                        )
        return carry

    lax.fori_loop(0, 4, along_z, 0)

    def along_y(t, carry):
        for z in range(4):
            for sx in range(2):
                low = [zs1[z, t, sx, 8 - i : 24 - i, :] for i in range(4)]
                high = [zs1[z, t, 2 + sx, 8 - i : 24 - i, :] for i in range(4)]
                fo[sx, z, t, pl.ds(0, 16, stride=2), :] = synthesis_pair(low, high, 0)
                fo[sx, z, t, pl.ds(1, 16, stride=2), :] = synthesis_pair(low, high, 1)
        return carry

    lax.fori_loop(0, 4, along_y, 0)
    loads[4].wait()
    both = jnp.concatenate([fo[0].reshape(512, 128), fo[1].reshape(512, 128)], axis=1)
    den[...] = product(both, a1t).reshape(4, 4, 32, 256)

    for copy in z_copies:
        copy.wait_recv()
    full = jnp.sum(arz[...], axis=0)
    cells = float(4 * 32 * 256 * total * 2)
    weights = jnp.where(lane[0:1] < 4, full[1:2], 1.0)
    gcv[...] = cells * full[0:1] / (weights * weights)
    for copy in sent:
        copy.wait_send()


def solution(mesh):
    nx, nz = 8, 16
    return on_grid(mesh, nx, nz)


def on_grid(mesh, nx, nz):
    split = Mesh(
        mesh.devices.reshape(mesh.shape["cube"], nx, nz, mesh.shape["gy"]),
        ("cube", "gz_0", "gz_1", "gy"),
    )
    full = in_two_parts(analysis_matrix(256))
    half = in_two_parts(analysis_matrix(128))
    matrices = (full, full.transpose(0, 2, 1), half, half.transpose(0, 2, 1))
    copies = 1 + 5 + 2 + 5 + 2 + (2 * nx - 1) + 2 + (nz - 1)
    f32 = jnp.float32

    def body(noisy_cube, thresholds):
        den, gcv = pl.pallas_call(
            functools.partial(kernel, nx, nz),
            out_shape=(
                jax.ShapeDtypeStruct((4, 4, 32, 256), f32),
                jax.ShapeDtypeStruct((1, 128), f32),
            ),
            in_specs=[pl.BlockSpec(memory_space=pltpu.SMEM)]
            + [pl.BlockSpec(memory_space=pl.ANY)] * 5,
            out_specs=(
                pl.BlockSpec(memory_space=pltpu.VMEM),
                pl.BlockSpec(memory_space=pltpu.VMEM),
            ),
            scratch_shapes=[
                pltpu.VMEM((4, 56, 256), f32),
                pltpu.VMEM((2, 4, 56, 128), f32),
                pltpu.VMEM((4, 24, 128), f32),
                pltpu.VMEM((4, 24, 128), f32),
                pltpu.VMEM((10, 4, 16, 128), f32),
                pltpu.VMEM((22, 2, 8, 128), f32),
                pltpu.VMEM((5, 7, 24, 128), f32),
                pltpu.VMEM((6, 2, 2, 16, 128), f32),
                pltpu.VMEM((4, 5, 2, 24, 128), f32),
                pltpu.VMEM((4, 5, 32, 128), f32),
                pltpu.VMEM((4, 5, 24, 128), f32),
                pltpu.VMEM((4, 4, 4, 24, 128), f32),
                pltpu.VMEM((2, 4, 4, 32, 128), f32),
                pltpu.VMEM((2, 256, 256), jnp.bfloat16),
                pltpu.VMEM((2, 256, 256), jnp.bfloat16),
                pltpu.VMEM((2, 128, 128), jnp.bfloat16),
                pltpu.VMEM((2, 128, 128), jnp.bfloat16),
                pltpu.VMEM((2, 128), f32),
                pltpu.VMEM((2, 128), f32),
                pltpu.VMEM((2 * nx, 2, 128), f32),
                pltpu.VMEM((nz, 2, 128), f32),
                pltpu.SemaphoreType.DMA((5,)),
                pltpu.SemaphoreType.DMA((copies,)),
                pltpu.SemaphoreType.DMA((copies,)),
                pltpu.SemaphoreType.REGULAR,
                pltpu.SemaphoreType.REGULAR,
                pltpu.SemaphoreType.REGULAR,
            ],
            compiler_params=pltpu.CompilerParams(collective_id=0, has_side_effects=True),
        )(thresholds, noisy_cube, *(jnp.asarray(m) for m in matrices))
        return den, gcv[0, 0:4]

    return jax.shard_map(
        body,
        mesh=split,
        in_specs=(P(CUBE_GZ, "gy", None), P()),
        out_specs=(P(CUBE_GZ, None, "gy", None), P("cube")),
        check_vma=False,
    )
```

```python
import functools

import jax
import jax.numpy as jnp
import numpy as np
from jax import lax
from jax.experimental import pallas as pl
from jax.experimental.pallas import tpu as pltpu
from jax.sharding import Mesh
from jax.sharding import PartitionSpec as P

MESH = pl.DeviceIdType.MESH
CUBE_GZ = ("cube", "gz_0", "gz_1")

LOWPASS = (
    0.2303778133088964,
    0.7148465705529155,
    0.6308807679298587,
    -0.0279837694168599,
    -0.1870348117190931,
    0.0308413818355607,
    0.0328830116668852,
    -0.010597401785069,
)
HIGHPASS = tuple(((-1) ** tap * LOWPASS[7 - tap] for tap in range(8)))


def composed(second):
    taps = np.zeros(22)
    for outer in range(8):
        for inner in range(8):
            taps[2 * outer + inner] += second[outer] * LOWPASS[inner]
    return tuple(float(tap) for tap in taps)


DEEP_LOW = composed(LOWPASS)
DEEP_HIGH = composed(HIGHPASS)


def analysis_matrix(length):
    matrix = np.zeros((length, length))
    for k in range(length // 2):
        for tap in range(8):
            matrix[(2 * k + tap) % length, k] += LOWPASS[tap]
            matrix[(2 * k + tap) % length, length // 2 + k] += HIGHPASS[tap]
    return matrix


def in_two_parts(matrix):
    exact = matrix.astype(np.float32)
    upper = exact.astype(jnp.bfloat16)
    lower = (exact - upper.astype(np.float32)).astype(jnp.bfloat16)
    return np.stack([upper, lower])


def product(values, parts):
    upper = values.astype(jnp.bfloat16)
    lower = (values - upper.astype(jnp.float32)).astype(jnp.bfloat16)
    dot = functools.partial(jnp.dot, preferred_element_type=jnp.float32)
    return dot(upper, parts[0]) + (dot(lower, parts[0]) + dot(upper, parts[1]))


def weighted(taps, values):
    result = taps[0] * values[0]
    for tap, value in zip(taps[1:], values[1:]):
        result = result + tap * value
    return result


def synthesis_pair(low, high, odd):
    return weighted(LOWPASS[odd::2], low) + weighted(HIGHPASS[odd::2], high)


def shrunk(values, limit):
    return values - jnp.clip(values, -limit, limit)


def kernel(
    nx,
    nz,
    thr_hbm,
    x_hbm,
    a1_hbm,
    a1t_hbm,
    a2t_hbm,
    den,
    gcv,
    thr,
    raw,
    xa,
    za,
    zb,
    part_out,
    part_in,
    da,
    db,
    cb,
    zs2,
    co,
    cr,
    zs1,
    fo,
    a1,
    a1t,
    a2t,
    row,
    tot,
    arx,
    arz,
    local_sem,
    send_sem,
    recv_sem,
    ready,
):
    cube, gx, gz, gy = (lax.axis_index(n) for n in ("cube", "gz_0", "gz_1", "gy"))
    total = nx * nz
    flat = gx * nz + gz
    other = 1 - gy
    other_core = (cube, gx, gz, other)

    def along(offset):
        place = lax.rem(flat + (offset + total), total)
        return (cube, lax.div(place, nz), lax.rem(place, nz), gy)

    def across_x(offset, core):
        return (cube, lax.rem(gx + (offset + nx), nx), gz, core)

    def across_z(offset):
        return (cube, gx, lax.rem(gz + offset, nz), gy)

    sent = []

    def send(src, dst, device):
        index = len(sent)
        copy = pltpu.make_async_remote_copy(
            src_ref=src,
            dst_ref=dst,
            send_sem=send_sem.at[index],
            recv_sem=recv_sem.at[index],
            device_id=device,
            device_id_type=MESH,
        )
        copy.start()
        sent.append(copy)
        return copy

    def signal(sem, *devices):
        for device in devices:
            pl.semaphore_signal(sem, inc=1, device_id=device, device_id_type=MESH)

    near_z, mid_z, far_z, near_x, mid_x, core = (ready.at[i] for i in range(6))

    loads = [pltpu.make_async_copy(x_hbm, raw.at[:, 0:32, :], local_sem.at[0])]
    for index, (src, dst) in enumerate(
        ((a1_hbm, a1), (thr_hbm, thr), (a2t_hbm, a2t), (a1t_hbm, a1t))
    ):
        loads.append(pltpu.make_async_copy(src, dst, local_sem.at[index + 1]))
    for load in loads:
        load.start()

    barrier = pltpu.get_barrier_semaphore()
    signal(
        barrier, other_core, along(1), along(-1), across_x(1, gy), across_x(-1, gy)
    )
    pl.semaphore_wait(barrier, 5)

    loads[0].wait()
    rows_copy = send(raw.at[:, 0:24, :], raw.at[:, 32:56, :], other_core)
    signal(near_z, along(1), along(-1))
    signal(near_x, across_x(1, gy), across_x(-1, gy))

    loads[1].wait()
    own = product(raw[:, 0:32, :].reshape(128, 256), a1)
    for band in range(3):
        xa[band, :, 0:32, :] = own[:, 128 * band : 128 * band + 128].reshape(4, 32, 128)
    pl.semaphore_wait(near_z, 2)
    signal(mid_z, along(2), along(-2))
    rows_copy.wait_recv()
    beyond = product(raw[:, 32:56, :].reshape(96, 256), a1)
    for band in range(3):
        xa[band, :, 32:56, :] = beyond[:, 128 * band : 128 * band + 128].reshape(4, 24, 128)

    deep = []
    for z in range(4):
        taps = [xa[2, z, pl.ds(i, 8, stride=4), :] for i in range(22)]
        deep.append((weighted(DEEP_LOW, taps), weighted(DEEP_HIGH, taps)))

    def partial(sz, sy, offset):
        filter_taps = (DEEP_LOW, DEEP_HIGH)[sz]
        planes = [z for z in range(4) if z + 8 - 4 * offset < 22]
        return weighted(
            [filter_taps[z + 8 - 4 * offset] for z in planes], [deep[z][sy] for z in planes]
        )

    part_copies = []
    for index, offset in enumerate((2, -2, -3, 1, -1)):
        for sz in range(2):
            for sy in range(2):
                part_out[index, sz, sy] = partial(sz, sy, offset)
        if offset == -3:
            pl.semaphore_wait(mid_z, 2)
        part_copies.append(send(part_out.at[index], part_in.at[index], along(offset)))

    for z in range(4):
        for sx in range(2):
            taps = [xa[sx, z, pl.ds(j, 16, stride=2), :] for j in range(8)]
            za[4 + z, sx] = weighted(LOWPASS, taps)
            zb[2 + z, sx] = weighted(HIGHPASS, taps)
    plane_copies = [
        send(za.at[4:8], za.at[0:4], along(1)),
        send(zb.at[2:6], zb.at[6:10], along(-1)),
        send(zb.at[4:6], zb.at[0:2], along(1)),
        send(za.at[4:6], za.at[8:10], along(-1)),
    ]
    signal(far_z, along(4), along(-4))
    pl.semaphore_wait(near_x, 2)
    signal(mid_x, across_x(2, gy), across_x(-2, gy))

    lane = lax.broadcasted_iota(jnp.int32, (8, 128), 1)
    first_half = lane < 64
    zero = jnp.zeros((8, 128), jnp.float32)
    loads[2].wait()
    limits = [thr[t] for t in range(4)]
    squares = [limit * limit for limit in limits]

    for copy in part_copies:
        copy.wait_recv()
    residual = [zero] * 4
    weight = [zero] * 4
    for sz in range(2):
        for sy in range(2):
            c = partial(sz, sy, 0)
            for index in range(5):
                c = c + part_in[index, sz, sy]
            cb[3, sz, sy, 8:16, :] = c
    coeff_copies = [
        send(cb.at[3, :, :, 8:16, :], cb.at[3 - offset, :, :, 8:16, :], along(offset))
        for offset in (3, -2, 2, -1, 1)
    ]
    for sz in range(2):
        for sy in range(2):
            c = cb[3, sz, sy, 8:16, :]
            square = c * c
            for t in range(4):
                cut = jnp.clip(c, -limits[t], limits[t])
                kept = squares[t] / (squares[t] + square)
                cut = cut * cut
                if sz == 0 and sy == 0:
                    cut = jnp.where(first_half, zero, cut)
                    kept = jnp.where(first_half, zero, kept)
                residual[t] = residual[t] + cut
                weight[t] = weight[t] + kept
    pl.semaphore_wait(mid_x, 2)
    signal(core, other_core)

    for copy in plane_copies:
        copy.wait_recv()
    for k in range(2):
        for sx in range(2):
            planes = [za[2 * k + j, sx] for j in range(8)]
            if sx:
                da[1 + k, 1, 8:24, :] = weighted(LOWPASS, planes)
            da[1 + k, 2 * sx, 8:24, :] = weighted(HIGHPASS, planes)
            planes = [zb[2 * k + j, sx] for j in range(8)]
            db[2 + k, 2 * sx, 8:24, :] = weighted(LOWPASS, planes)
            db[2 + k, 2 * sx + 1, 8:24, :] = weighted(HIGHPASS, planes)
    detail_copies = [
        send(da.at[1:3, :, 8:24, :], da.at[3:5, :, 8:24, :], along(-1)),
        send(db.at[2:4, :, 8:24, :], db.at[0:2, :, 8:24, :], along(1)),
        send(db.at[2, :, 8:24, :], db.at[4, :, 8:24, :], along(-1)),
        send(da.at[2, :, 8:24, :], da.at[0, :, 8:24, :], along(1)),
    ]

    def add_bands(ref, first):
        def add_band(band, sums):
            sums = list(sums)
            for k in range(2):
                for half in range(2):
                    c = ref[first + k, band, 8 + 8 * half : 16 + 8 * half, :]
                    square = c * c
                    for t in range(4):
                        cut = jnp.clip(c, -limits[t], limits[t])
                        sums[t] = sums[t] + cut * cut
                        sums[4 + t] = sums[4 + t] + squares[t] / (squares[t] + square)
            return tuple(sums)

        return add_band

    sums = lax.fori_loop(0, 3, add_bands(da, 1), tuple(residual + weight))
    sums = lax.fori_loop(0, 4, add_bands(db, 2), sums)

    def as_row(parts):
        line = jnp.zeros((1, 128), jnp.float32)
        for t, part in enumerate(parts):
            value = jnp.sum(jnp.sum(part, axis=0, keepdims=True), axis=1, keepdims=True)
            line = jnp.where(lane[0:1] == t, value, line)
        return line

    row[0:1, :] = as_row(sums[0:4])
    row[1:2, :] = as_row(sums[4:8])
    slot = gy * nx + gx
    arx[pl.ds(slot, 1)] = row[...].reshape(1, 2, 128)
    pl.semaphore_wait(core, 1)
    pl.semaphore_wait(far_z, 2)
    x_copies = [
        send(row, arx.at[slot], across_x(offset, place))
        for offset in sorted(range(nx), key=lambda o: -min(o, nx - o))
        for place in (gy, other)
        if not (place is gy and offset == 0)
    ]

    for copy in detail_copies:
        copy.wait_recv()
    detail_rows = [
        send(da.at[:, :, 16:24, :], da.at[:, :, 0:8, :], other_core),
        send(db.at[:, :, 16:24, :], db.at[:, :, 0:8, :], other_core),
    ]

    for copy in detail_rows:
        copy.wait_recv()

    def along_z(t, carry):
        limit = thr[t]
        for part in range(3):
            rows = slice(8 * part, 8 * part + 8)

            def cut(ref, band):
                return [shrunk(ref[k, band, rows, :], limit) for k in range(5)]

            pairs = (
                (None, cut(da, 0)),
                (cut(da, 1), cut(da, 2)),
                (cut(db, 0), cut(db, 1)),
                (cut(db, 2), cut(db, 3)),
            )
            for band, (low, high) in enumerate(pairs):
                for e in range(2):
                    order = [3 + e - i for i in range(4)]
                    for odd in range(2):
                        value = weighted(HIGHPASS[odd::2], [high[i] for i in order])
                        if low is not None:
                            value = value + weighted(LOWPASS[odd::2], [low[i] for i in order])
                        zs1[2 * e + odd, t, band, rows, :] = value
        return carry

    lax.fori_loop(0, 4, along_z, 0)

    for copy in coeff_copies:
        copy.wait_recv()
    deep_rows = send(cb.at[:, :, :, 8:16, :], cb.at[:, :, :, 0:8, :], other_core)

    for copy in x_copies:
        copy.wait_recv()
    tot[...] = jnp.sum(arx[...], axis=0)
    arz[pl.ds(gz, 1)] = tot[...].reshape(1, 2, 128)
    z_copies = [
        send(tot, arz.at[gz], across_z(offset))
        for offset in sorted(range(1, nz), key=lambda o: min(o, nz - o))
    ]

    deep_rows.wait_recv()

    def deep_along_z(t, carry):
        limit = thr[t]
        for sy in range(2):
            for part in range(2):
                bands = []
                for sz in range(2):
                    values = []
                    for m in range(6):
                        c = cb[m, sz, sy, 8 * part : 8 * part + 8, :]
                        s = shrunk(c, limit)
                        values.append(jnp.where(first_half, c, s) if sz + sy == 0 else s)
                    bands.append(values)
                for k in range(5):
                    p = 3 + (k + 1) // 2
                    odd = (k + 1) % 2
                    order = [p - i for i in range(4)]
                    zs2[t, k, sy, 8 + 8 * part : 16 + 8 * part, :] = synthesis_pair(
                        [bands[0][i] for i in order], [bands[1][i] for i in order], odd
                    )
        return carry

    lax.fori_loop(0, 4, deep_along_z, 0)

    def deep_along_y(t, carry):
        for k in range(5):
            low = [zs2[t, k, 0, 8 - i : 24 - i, :] for i in range(4)]
            high = [zs2[t, k, 1, 8 - i : 24 - i, :] for i in range(4)]
            co[t, k, pl.ds(0, 16, stride=2), :] = synthesis_pair(low, high, 0)
            co[t, k, pl.ds(1, 16, stride=2), :] = synthesis_pair(low, high, 1)
        return carry

    lax.fori_loop(0, 4, deep_along_y, 0)
    loads[3].wait()
    cr[...] = product(co[:, :, 8:32, :].reshape(480, 128), a2t).reshape(4, 5, 24, 128)

    def along_y(t, carry):
        for part in range(3):
            rows = slice(8 * part, 8 * part + 8)
            low = [cr[t, k, rows, :] for k in range(5)]
            for e in range(2):
                order = [3 + e - i for i in range(4)]
                for odd in range(2):
                    zs1[2 * e + odd, t, 0, rows, :] = zs1[
                        2 * e + odd, t, 0, rows, :
                    ] + weighted(LOWPASS[odd::2], [low[i] for i in order])
        for z in range(4):
            for sx in range(2):
                low = [zs1[z, t, sx, 8 - i : 24 - i, :] for i in range(4)]
                high = [zs1[z, t, 2 + sx, 8 - i : 24 - i, :] for i in range(4)]
                fo[sx, z, t, pl.ds(0, 16, stride=2), :] = synthesis_pair(low, high, 0)
                fo[sx, z, t, pl.ds(1, 16, stride=2), :] = synthesis_pair(low, high, 1)
        return carry

    lax.fori_loop(0, 4, along_y, 0)
    loads[4].wait()
    both = jnp.concatenate([fo[0].reshape(512, 128), fo[1].reshape(512, 128)], axis=1)
    den[...] = product(both, a1t).reshape(4, 4, 32, 256)

    for copy in z_copies:
        copy.wait_recv()
    full = jnp.sum(arz[...], axis=0)
    cells = float(4 * 32 * 256 * total * 2)
    weights = jnp.where(lane[0:1] < 4, full[1:2], 1.0)
    gcv[...] = cells * full[0:1] / (weights * weights)
    for copy in sent:
        copy.wait_send()


def solution(mesh):
    nx, nz = 8, 16
    return on_grid(mesh, nx, nz)


def on_grid(mesh, nx, nz):
    split = Mesh(
        mesh.devices.reshape(mesh.shape["cube"], nx, nz, mesh.shape["gy"]),
        ("cube", "gz_0", "gz_1", "gy"),
    )
    first = analysis_matrix(256)
    second = analysis_matrix(128)
    forward = np.concatenate([first, first[:, 0:128] @ second], axis=1)
    matrices = [in_two_parts(m) for m in (forward, first.T, second.T)]
    copies = 1 + 5 + 4 + 5 + 4 + (2 * nx - 1) + 2 + 1 + (nz - 1)
    f32 = jnp.float32

    def body(noisy_cube, thresholds):
        den, gcv = pl.pallas_call(
            functools.partial(kernel, nx, nz),
            out_shape=(
                jax.ShapeDtypeStruct((4, 4, 32, 256), f32),
                jax.ShapeDtypeStruct((1, 128), f32),
            ),
            in_specs=[pl.BlockSpec(memory_space=pltpu.HBM)] * 5,
            out_specs=(
                pl.BlockSpec(memory_space=pltpu.VMEM),
                pl.BlockSpec(memory_space=pltpu.VMEM),
            ),
            scratch_shapes=[
                pltpu.SMEM((4,), f32),
                pltpu.VMEM((4, 56, 256), f32),
                pltpu.VMEM((3, 4, 56, 128), f32),
                pltpu.VMEM((10, 2, 16, 128), f32),
                pltpu.VMEM((10, 2, 16, 128), f32),
                pltpu.VMEM((5, 2, 2, 8, 128), f32),
                pltpu.VMEM((5, 2, 2, 8, 128), f32),
                pltpu.VMEM((5, 3, 24, 128), f32),
                pltpu.VMEM((5, 4, 24, 128), f32),
                pltpu.VMEM((6, 2, 2, 16, 128), f32),
                pltpu.VMEM((4, 5, 2, 24, 128), f32),
                pltpu.VMEM((4, 5, 32, 128), f32),
                pltpu.VMEM((4, 5, 24, 128), f32),
                pltpu.VMEM((4, 4, 4, 24, 128), f32),
                pltpu.VMEM((2, 4, 4, 32, 128), f32),
                pltpu.VMEM((2, 256, 384), jnp.bfloat16),
                pltpu.VMEM((2, 256, 256), jnp.bfloat16),
                pltpu.VMEM((2, 128, 128), jnp.bfloat16),
                pltpu.VMEM((2, 128), f32),
                pltpu.VMEM((2, 128), f32),
                pltpu.VMEM((2 * nx, 2, 128), f32),
                pltpu.VMEM((nz, 2, 128), f32),
                pltpu.SemaphoreType.DMA((5,)),
                pltpu.SemaphoreType.DMA((copies,)),
                pltpu.SemaphoreType.DMA((copies,)),
                pltpu.SemaphoreType.REGULAR((6,)),
            ],
            compiler_params=pltpu.CompilerParams(
                collective_id=0, has_side_effects=True, vmem_limit_bytes=12 * 1024 * 1024
            ),
        )(thresholds, noisy_cube, *(jnp.asarray(m) for m in matrices))
        return den, gcv[0, 0:4]

    return jax.shard_map(
        body,
        mesh=split,
        in_specs=(P(CUBE_GZ, "gy", None), P()),
        out_specs=(P(CUBE_GZ, None, "gy", None), P("cube")),
        check_vma=False,
    )
```

```python
import functools

import jax
import jax.numpy as jnp
import numpy as np
from jax import lax
from jax.experimental import pallas as pl
from jax.experimental.pallas import tpu as pltpu
from jax.sharding import Mesh
from jax.sharding import PartitionSpec as P

MESH = pl.DeviceIdType.MESH
CUBE_GZ = ("cube", "gz_0", "gz_1")

LOWPASS = (
    0.2303778133088964,
    0.7148465705529155,
    0.6308807679298587,
    -0.0279837694168599,
    -0.1870348117190931,
    0.0308413818355607,
    0.0328830116668852,
    -0.010597401785069,
)
HIGHPASS = tuple(((-1) ** tap * LOWPASS[7 - tap] for tap in range(8)))


def composed(second):
    taps = np.zeros(22)
    for outer in range(8):
        for inner in range(8):
            taps[2 * outer + inner] += second[outer] * LOWPASS[inner]
    return tuple(float(tap) for tap in taps)


DEEP_LOW = composed(LOWPASS)
DEEP_HIGH = composed(HIGHPASS)


def analysis_matrix(length):
    matrix = np.zeros((length, length))
    for k in range(length // 2):
        for tap in range(8):
            matrix[(2 * k + tap) % length, k] += LOWPASS[tap]
            matrix[(2 * k + tap) % length, length // 2 + k] += HIGHPASS[tap]
    return matrix


def in_two_parts(matrix):
    exact = matrix.astype(np.float32)
    upper = exact.astype(jnp.bfloat16)
    lower = (exact - upper.astype(np.float32)).astype(jnp.bfloat16)
    return np.stack([upper, lower])


def product(values, parts):
    upper = values.astype(jnp.bfloat16)
    lower = (values - upper.astype(jnp.float32)).astype(jnp.bfloat16)
    dot = functools.partial(jnp.dot, preferred_element_type=jnp.float32)
    return dot(upper, parts[0]) + (dot(lower, parts[0]) + dot(upper, parts[1]))


def weighted(taps, values):
    result = taps[0] * values[0]
    for tap, value in zip(taps[1:], values[1:]):
        result = result + tap * value
    return result


def synthesis_pair(low, high, odd):
    return weighted(LOWPASS[odd::2], low) + weighted(HIGHPASS[odd::2], high)


def shrunk(values, limit):
    return values - jnp.clip(values, -limit, limit)


def kernel(
    nx,
    nz,
    thr_hbm,
    x_hbm,
    a1_hbm,
    a1t_hbm,
    a2t_hbm,
    den,
    gcv,
    thr,
    raw,
    xa,
    zw,
    part_out,
    part_in,
    db,
    cb,
    zs2,
    co,
    cr,
    zs1,
    fo,
    a1,
    a1t,
    a2t,
    row,
    tot,
    arx,
    arz,
    local_sem,
    send_sem,
    recv_sem,
    link,
    near,
    mid,
):
    cube, gx, gz, gy = (lax.axis_index(n) for n in ("cube", "gz_0", "gz_1", "gy"))
    total = nx * nz
    flat = gx * nz + gz
    other = 1 - gy
    other_core = (cube, gx, gz, other)

    def along(offset):
        place = lax.rem(flat + (offset + total), total)
        return (cube, lax.div(place, nz), lax.rem(place, nz), gy)

    def across_x(offset, core):
        return (cube, lax.rem(gx + (offset + nx), nx), gz, core)

    def across_z(offset):
        return (cube, gx, lax.rem(gz + offset, nz), gy)

    groups = []

    def send_all(whole, *copies):
        index = len(groups)
        sems = (send_sem.at[index], recv_sem.at[index])
        for src, dst, device in copies:
            pltpu.make_async_remote_copy(
                src_ref=src,
                dst_ref=dst,
                send_sem=sems[0],
                recv_sem=sems[1],
                device_id=device,
                device_id_type=MESH,
            ).start()
        group = pltpu.make_async_remote_copy(
            src_ref=whole,
            dst_ref=whole,
            send_sem=sems[0],
            recv_sem=sems[1],
            device_id=other_core,
            device_id_type=MESH,
        )
        groups.append(group)
        return group

    def signal(sem, *devices):
        for device in devices:
            pl.semaphore_signal(sem, inc=1, device_id=device, device_id_type=MESH)

    loads = [pltpu.make_async_copy(x_hbm, raw.at[:, 0:32, :], local_sem.at[0])]
    for index, (src, dst) in enumerate(
        ((a1_hbm, a1), (thr_hbm, thr), (a2t_hbm, a2t), (a1t_hbm, a1t))
    ):
        loads.append(pltpu.make_async_copy(src, dst, local_sem.at[index + 1]))
    for load in loads:
        load.start()

    barrier = pltpu.get_barrier_semaphore()

    @pl.when(gy == 0)
    def _():
        signal(barrier, other_core)

    @pl.when(gy == 1)
    def _():
        pl.semaphore_wait(barrier, 1)
        signal(link, other_core)

    @pl.when(gy == 0)
    def _():
        pl.semaphore_wait(link, 1)
        signal(barrier, *(along(offset) for offset in (1, -1, 2, -2, 3, -3)))
        signal(barrier, across_x(1, gy), across_x(-1, gy))

    loads[0].wait()
    rows_copy = send_all(
        raw.at[:, 0:24, :], (raw.at[:, 0:24, :], raw.at[:, 32:56, :], other_core)
    )

    loads[1].wait()
    own = product(raw[:, 0:32, :].reshape(128, 256), a1)
    for band in range(3):
        xa[band, :, 0:32, :] = own[:, 128 * band : 128 * band + 128].reshape(4, 32, 128)
    rows_copy.wait_recv()
    beyond = product(raw[:, 32:56, :].reshape(96, 256), a1)
    for band in range(3):
        xa[band, :, 32:56, :] = beyond[:, 128 * band : 128 * band + 128].reshape(4, 24, 128)

    deep = []
    for z in range(4):
        taps = [xa[2, z, pl.ds(i, 8, stride=4), :] for i in range(22)]
        deep.append((weighted(DEEP_LOW, taps), weighted(DEEP_HIGH, taps)))

    def partial(sz, sy, offset):
        filter_taps = (DEEP_LOW, DEEP_HIGH)[sz]
        planes = [z for z in range(4) if z + 8 - 4 * offset < 22]
        return weighted(
            [filter_taps[z + 8 - 4 * offset] for z in planes], [deep[z][sy] for z in planes]
        )

    offsets = (2, -2, -3, 1, -1)
    for index, offset in enumerate(offsets):
        for sz in range(2):
            for sy in range(2):
                part_out[index, sz, sy] = partial(sz, sy, offset)

    @pl.when(gy == 0)
    def _():
        pl.semaphore_wait(barrier, 8)
        signal(link, other_core)

    @pl.when(gy == 1)
    def _():
        pl.semaphore_wait(link, 1)

    part_copies = send_all(
        part_in,
        *(
            (part_out.at[index], part_in.at[index], along(offset))
            for index, offset in enumerate(offsets)
        ),
    )

    for z in range(4):
        for sx in range(2):
            taps = [xa[sx, z, pl.ds(j, 16, stride=2), :] for j in range(8)]
            zw[6 + z, sx] = weighted(LOWPASS, taps)
            zw[6 + z, 2 + sx] = weighted(HIGHPASS, taps)
    six = zw.at[0:6]
    plane_copies = send_all(
        six,
        (zw.at[6:10, 0:2], zw.at[2:6, 0:2], along(1)),
        (zw.at[6:10, 2:4], zw.at[10:14, 2:4], along(-1)),
        (zw.at[8:10, 2:4], zw.at[4:6, 2:4], along(1)),
        (zw.at[6:8, 0:2], zw.at[10:12, 0:2], along(-1)),
    )
    more_copies = send_all(
        six,
        (zw.at[8:10], zw.at[0:2], along(2)),
        (zw.at[6:8], zw.at[14:16], along(-2)),
        (zw.at[6:8, 2:4], zw.at[2:4, 2:4], along(1)),
        (zw.at[8:10, 0:2], zw.at[12:14, 0:2], along(-1)),
    )

    @pl.when(gy == 0)
    def _():
        signal(near, along(3), along(-3), across_x(1, gy), across_x(-1, gy))
        pl.semaphore_wait(near, 4)
        signal(mid, along(2), along(-2), across_x(2, gy), across_x(-2, gy))

    lane = lax.broadcasted_iota(jnp.int32, (8, 128), 1)
    first_half = lane < 64
    zero = jnp.zeros((8, 128), jnp.float32)
    loads[2].wait()
    limits = [thr[t] for t in range(4)]
    squares = [limit * limit for limit in limits]

    part_copies.wait_recv()
    residual = [zero] * 4
    weight = [zero] * 4
    for sz in range(2):
        for sy in range(2):
            c = partial(sz, sy, 0)
            for index in range(5):
                c = c + part_in[index, sz, sy]
            cb[3, sz, sy, 8:16, :] = c
    coeff_copies = send_all(
        cb.at[0:5, :, :, 8:16, :],
        *(
            (cb.at[3, :, :, 8:16, :], cb.at[3 - offset, :, :, 8:16, :], along(offset))
            for offset in (3, -2, 2, -1, 1)
        ),
    )
    for sz in range(2):
        for sy in range(2):
            c = cb[3, sz, sy, 8:16, :]
            square = c * c
            for t in range(4):
                cut = jnp.clip(c, -limits[t], limits[t])
                kept = squares[t] / (squares[t] + square)
                cut = cut * cut
                if sz == 0 and sy == 0:
                    cut = jnp.where(first_half, zero, cut)
                    kept = jnp.where(first_half, zero, kept)
                residual[t] = residual[t] + cut
                weight[t] = weight[t] + kept

    def level_one(k, half):
        for sx in range(2):
            band = 2 * half + sx
            planes = [zw[2 * k + j, band] for j in range(8)]
            if band:
                db[k, 2 * band - 1, 8:24, :] = weighted(LOWPASS, planes)
            db[k, 2 * band, 8:24, :] = weighted(HIGHPASS, planes)

    plane_copies.wait_recv()
    for k in range(2):
        level_one(1 + k, 0)
        level_one(2 + k, 1)

    def add_bands(first):
        def add_band(band, sums):
            sums = list(sums)
            for k in range(2):
                for half in range(2):
                    c = db[first + k, band, 8 + 8 * half : 16 + 8 * half, :]
                    square = c * c
                    for t in range(4):
                        cut = jnp.clip(c, -limits[t], limits[t])
                        sums[t] = sums[t] + cut * cut
                        sums[4 + t] = sums[4 + t] + squares[t] / (squares[t] + square)
            return tuple(sums)

        return add_band

    sums = lax.fori_loop(0, 3, add_bands(1), tuple(residual + weight))
    sums = lax.fori_loop(3, 7, add_bands(2), sums)

    def as_row(parts):
        line = jnp.zeros((1, 128), jnp.float32)
        for t, part in enumerate(parts):
            value = jnp.sum(jnp.sum(part, axis=0, keepdims=True), axis=1, keepdims=True)
            line = jnp.where(lane[0:1] == t, value, line)
        return line

    row[0:1, :] = as_row(sums[0:4])
    row[1:2, :] = as_row(sums[4:8])
    slot = gy * nx + gx
    arx[pl.ds(slot, 1)] = row[...].reshape(1, 2, 128)

    @pl.when(gy == 0)
    def _():
        pl.semaphore_wait(mid, 4)
        signal(link, other_core)

    @pl.when(gy == 1)
    def _():
        pl.semaphore_wait(link, 1)

    x_copies = send_all(
        arx.at[0 : 2 * nx - 1],
        *(
            (row, arx.at[slot], across_x(offset, place))
            for offset in sorted(range(nx), key=lambda o: -min(o, nx - o))
            for place in (gy, other)
            if not (place is gy and offset == 0)
        ),
    )

    more_copies.wait_recv()
    for k in range(5):
        for half in range(2):
            if k - half not in (1, 2):
                level_one(k, half)

    detail_rows = send_all(
        db.at[:, :, 16:24, :], (db.at[:, :, 16:24, :], db.at[:, :, 0:8, :], other_core)
    )
    detail_rows.wait_recv()

    def along_z(t, carry):
        limit = thr[t]
        for part in range(3):
            rows = slice(8 * part, 8 * part + 8)

            def cut(band):
                return [shrunk(db[k, band, rows, :], limit) for k in range(5)]

            pairs = ((None, cut(0)), (cut(1), cut(2)), (cut(3), cut(4)), (cut(5), cut(6)))
            for band, (low, high) in enumerate(pairs):
                for e in range(2):
                    order = [3 + e - i for i in range(4)]
                    for odd in range(2):
                        value = weighted(HIGHPASS[odd::2], [high[i] for i in order])
                        if low is not None:
                            value = value + weighted(LOWPASS[odd::2], [low[i] for i in order])
                        zs1[2 * e + odd, t, band, rows, :] = value
        return carry

    lax.fori_loop(0, 4, along_z, 0)

    coeff_copies.wait_recv()
    deep_rows = send_all(
        cb.at[:, :, :, 8:16, :],
        (cb.at[:, :, :, 8:16, :], cb.at[:, :, :, 0:8, :], other_core),
    )

    x_copies.wait_recv()
    tot[...] = jnp.sum(arx[...], axis=0)
    arz[pl.ds(gz, 1)] = tot[...].reshape(1, 2, 128)
    z_copies = send_all(
        arz.at[0 : nz - 1],
        *(
            (tot, arz.at[gz], across_z(offset))
            for offset in sorted(range(1, nz), key=lambda o: min(o, nz - o))
        ),
    )

    deep_rows.wait_recv()

    def deep_along_z(t, carry):
        limit = thr[t]
        for sy in range(2):
            for part in range(2):
                bands = []
                for sz in range(2):
                    values = []
                    for m in range(6):
                        c = cb[m, sz, sy, 8 * part : 8 * part + 8, :]
                        s = shrunk(c, limit)
                        values.append(jnp.where(first_half, c, s) if sz + sy == 0 else s)
                    bands.append(values)
                for k in range(5):
                    p = 3 + (k + 1) // 2
                    odd = (k + 1) % 2
                    order = [p - i for i in range(4)]
                    zs2[t, k, sy, 8 + 8 * part : 16 + 8 * part, :] = synthesis_pair(
                        [bands[0][i] for i in order], [bands[1][i] for i in order], odd
                    )
        return carry

    lax.fori_loop(0, 4, deep_along_z, 0)

    def deep_along_y(t, carry):
        for k in range(5):
            low = [zs2[t, k, 0, 8 - i : 24 - i, :] for i in range(4)]
            high = [zs2[t, k, 1, 8 - i : 24 - i, :] for i in range(4)]
            co[t, k, pl.ds(0, 16, stride=2), :] = synthesis_pair(low, high, 0)
            co[t, k, pl.ds(1, 16, stride=2), :] = synthesis_pair(low, high, 1)
        return carry

    lax.fori_loop(0, 4, deep_along_y, 0)
    loads[3].wait()
    cr[...] = product(co[:, :, 8:32, :].reshape(480, 128), a2t).reshape(4, 5, 24, 128)

    def along_y(t, carry):
        for part in range(3):
            rows = slice(8 * part, 8 * part + 8)
            low = [cr[t, k, rows, :] for k in range(5)]
            for e in range(2):
                order = [3 + e - i for i in range(4)]
                for odd in range(2):
                    zs1[2 * e + odd, t, 0, rows, :] = zs1[
                        2 * e + odd, t, 0, rows, :
                    ] + weighted(LOWPASS[odd::2], [low[i] for i in order])
        for z in range(4):
            for sx in range(2):
                low = [zs1[z, t, sx, 8 - i : 24 - i, :] for i in range(4)]
                high = [zs1[z, t, 2 + sx, 8 - i : 24 - i, :] for i in range(4)]
                fo[sx, z, t, pl.ds(0, 16, stride=2), :] = synthesis_pair(low, high, 0)
                fo[sx, z, t, pl.ds(1, 16, stride=2), :] = synthesis_pair(low, high, 1)
        return carry

    lax.fori_loop(0, 4, along_y, 0)
    loads[4].wait()
    both = jnp.concatenate([fo[0].reshape(512, 128), fo[1].reshape(512, 128)], axis=1)
    den[...] = product(both, a1t).reshape(4, 4, 32, 256)

    z_copies.wait_recv()
    full = jnp.sum(arz[...], axis=0)
    cells = float(4 * 32 * 256 * total * 2)
    weights = jnp.where(lane[0:1] < 4, full[1:2], 1.0)
    gcv[...] = cells * full[0:1] / (weights * weights)
    for group in groups:
        group.wait_send()


def solution(mesh):
    nx, nz = 8, 16
    return on_grid(mesh, nx, nz)


def on_grid(mesh, nx, nz):
    split = Mesh(
        mesh.devices.reshape(mesh.shape["cube"], nx, nz, mesh.shape["gy"]),
        ("cube", "gz_0", "gz_1", "gy"),
    )
    first = analysis_matrix(256)
    second = analysis_matrix(128)
    forward = np.concatenate([first, first[:, 0:128] @ second], axis=1)
    matrices = [in_two_parts(m) for m in (forward, first.T, second.T)]
    f32 = jnp.float32

    def body(noisy_cube, thresholds):
        den, gcv = pl.pallas_call(
            functools.partial(kernel, nx, nz),
            out_shape=(
                jax.ShapeDtypeStruct((4, 4, 32, 256), f32),
                jax.ShapeDtypeStruct((1, 128), f32),
            ),
            in_specs=[pl.BlockSpec(memory_space=pltpu.HBM)] * 5,
            out_specs=(
                pl.BlockSpec(memory_space=pltpu.VMEM),
                pl.BlockSpec(memory_space=pltpu.VMEM),
            ),
            scratch_shapes=[
                pltpu.SMEM((4,), f32),
                pltpu.VMEM((4, 56, 256), f32),
                pltpu.VMEM((3, 4, 56, 128), f32),
                pltpu.VMEM((16, 4, 16, 128), f32),
                pltpu.VMEM((5, 2, 2, 8, 128), f32),
                pltpu.VMEM((5, 2, 2, 8, 128), f32),
                pltpu.VMEM((5, 7, 24, 128), f32),
                pltpu.VMEM((6, 2, 2, 16, 128), f32),
                pltpu.VMEM((4, 5, 2, 24, 128), f32),
                pltpu.VMEM((4, 5, 32, 128), f32),
                pltpu.VMEM((4, 5, 24, 128), f32),
                pltpu.VMEM((4, 4, 4, 24, 128), f32),
                pltpu.VMEM((2, 4, 4, 32, 128), f32),
                pltpu.VMEM((2, 256, 384), jnp.bfloat16),
                pltpu.VMEM((2, 256, 256), jnp.bfloat16),
                pltpu.VMEM((2, 128, 128), jnp.bfloat16),
                pltpu.VMEM((2, 128), f32),
                pltpu.VMEM((2, 128), f32),
                pltpu.VMEM((2 * nx, 2, 128), f32),
                pltpu.VMEM((nz, 2, 128), f32),
                pltpu.SemaphoreType.DMA((5,)),
                pltpu.SemaphoreType.DMA((9,)),
                pltpu.SemaphoreType.DMA((9,)),
                pltpu.SemaphoreType.REGULAR,
                pltpu.SemaphoreType.REGULAR,
                pltpu.SemaphoreType.REGULAR,
            ],
            compiler_params=pltpu.CompilerParams(
                collective_id=0, has_side_effects=True, vmem_limit_bytes=12 * 1024 * 1024
            ),
        )(*(pltpu.with_memory_space_constraint(v, pltpu.HBM) for v in (thresholds, noisy_cube, *(jnp.asarray(m) for m in matrices))))
        return den, gcv[0, 0:4]

    return jax.shard_map(
        body,
        mesh=split,
        in_specs=(P(CUBE_GZ, "gy", None), P()),
        out_specs=(P(CUBE_GZ, None, "gy", None), P("cube")),
        check_vma=False,
    )
```

```python
import functools

import jax
import jax.numpy as jnp
import numpy as np
from jax import lax
from jax.experimental import pallas as pl
from jax.experimental.pallas import tpu as pltpu
from jax.sharding import Mesh
from jax.sharding import PartitionSpec as P

MESH = pl.DeviceIdType.MESH
CUBE_GZ = ("cube", "gz_0", "gz_1")

LOWPASS = (
    0.2303778133088964,
    0.7148465705529155,
    0.6308807679298587,
    -0.0279837694168599,
    -0.1870348117190931,
    0.0308413818355607,
    0.0328830116668852,
    -0.010597401785069,
)
HIGHPASS = tuple(((-1) ** tap * LOWPASS[7 - tap] for tap in range(8)))


def composed(second):
    taps = np.zeros(22)
    for outer in range(8):
        for inner in range(8):
            taps[2 * outer + inner] += second[outer] * LOWPASS[inner]
    return tuple(float(tap) for tap in taps)


DEEP_LOW = composed(LOWPASS)
DEEP_HIGH = composed(HIGHPASS)


def analysis_matrix(length):
    matrix = np.zeros((length, length))
    for k in range(length // 2):
        for tap in range(8):
            matrix[(2 * k + tap) % length, k] += LOWPASS[tap]
            matrix[(2 * k + tap) % length, length // 2 + k] += HIGHPASS[tap]
    return matrix


def in_two_parts(matrix):
    exact = matrix.astype(np.float32)
    upper = exact.astype(jnp.bfloat16)
    lower = (exact - upper.astype(np.float32)).astype(jnp.bfloat16)
    return np.stack([upper, lower])


def product(values, parts):
    upper = values.astype(jnp.bfloat16)
    lower = (values - upper.astype(jnp.float32)).astype(jnp.bfloat16)
    dot = functools.partial(jnp.dot, preferred_element_type=jnp.float32)
    return dot(upper, parts[0]) + (dot(lower, parts[0]) + dot(upper, parts[1]))


def weighted(taps, values):
    result = taps[0] * values[0]
    for tap, value in zip(taps[1:], values[1:]):
        result = result + tap * value
    return result


def synthesis_pair(low, high, odd):
    return weighted(LOWPASS[odd::2], low) + weighted(HIGHPASS[odd::2], high)


def shrunk(values, limit):
    return values - jnp.clip(values, -limit, limit)


def kernel(
    nx,
    nz,
    thr_hbm,
    x_hbm,
    a1_hbm,
    a1t_hbm,
    a2t_hbm,
    den,
    gcv,
    thr,
    raw,
    xa,
    zw,
    part_out,
    part_in,
    db,
    cb,
    zs2,
    co,
    cr,
    zs1,
    fo,
    a1,
    a1t,
    a2t,
    row,
    tot,
    arx,
    arz,
    local_sem,
    send_sem,
    recv_sem,
    link,
    near,
    mid,
):
    cube, gx, gz, gy = (lax.axis_index(n) for n in ("cube", "gz_0", "gz_1", "gy"))
    total = nx * nz
    flat = gx * nz + gz
    other = 1 - gy
    other_core = (cube, gx, gz, other)

    def along(offset, core=None):
        place = lax.rem(flat + (offset + total), total)
        return (cube, lax.div(place, nz), lax.rem(place, nz), gy if core is None else core)

    def across_x(offset, core):
        return (cube, lax.rem(gx + (offset + nx), nx), gz, core)

    def across_z(offset):
        return (cube, gx, lax.rem(gz + offset, nz), gy)

    groups = []

    def send_all(whole, *copies):
        index = len(groups)
        sems = (send_sem.at[index], recv_sem.at[index])
        for src, dst, device in copies:
            pltpu.make_async_remote_copy(
                src_ref=src,
                dst_ref=dst,
                send_sem=sems[0],
                recv_sem=sems[1],
                device_id=device,
                device_id_type=MESH,
            ).start()
        group = pltpu.make_async_remote_copy(
            src_ref=whole,
            dst_ref=whole,
            send_sem=sems[0],
            recv_sem=sems[1],
            device_id=other_core,
            device_id_type=MESH,
        )
        groups.append(group)
        return group

    def signal(sem, *devices):
        for device in devices:
            pl.semaphore_signal(sem, inc=1, device_id=device, device_id_type=MESH)

    loads = [pltpu.make_async_copy(x_hbm, raw.at[:, 0:32, :], local_sem.at[0])]
    for index, (src, dst) in enumerate(
        ((a1_hbm, a1), (thr_hbm, thr), (a2t_hbm, a2t), (a1t_hbm, a1t))
    ):
        loads.append(pltpu.make_async_copy(src, dst, local_sem.at[index + 1]))
    for load in loads:
        load.start()

    barrier = pltpu.get_barrier_semaphore()

    @pl.when(gy == 0)
    def _():
        signal(barrier, other_core)

    around = [along(offset, 0) for offset in (3, -3, 2, -2, 1, -1)]
    signal(barrier, *around, across_x(1, 0), across_x(-1, 0))

    @pl.when(gy == 1)
    def _():
        pl.semaphore_wait(barrier, 1)
        signal(link, other_core)

    @pl.when(gy == 0)
    def _():
        pl.semaphore_wait(link, 1)

    loads[0].wait()
    rows_copy = send_all(
        raw.at[:, 0:24, :], (raw.at[:, 0:24, :], raw.at[:, 32:56, :], other_core)
    )

    loads[1].wait()
    own = product(raw[:, 0:32, :].reshape(128, 256), a1)
    for band in range(3):
        xa[band, :, 0:32, :] = own[:, 128 * band : 128 * band + 128].reshape(4, 32, 128)
    rows_copy.wait_recv()
    beyond = product(raw[:, 32:56, :].reshape(96, 256), a1)
    for band in range(3):
        xa[band, :, 32:56, :] = beyond[:, 128 * band : 128 * band + 128].reshape(4, 24, 128)

    deep = []
    for z in range(4):
        taps = [xa[2, z, pl.ds(i, 8, stride=4), :] for i in range(22)]
        deep.append((weighted(DEEP_LOW, taps), weighted(DEEP_HIGH, taps)))

    def partial(sz, sy, offset):
        filter_taps = (DEEP_LOW, DEEP_HIGH)[sz]
        planes = [z for z in range(4) if z + 8 - 4 * offset < 22]
        return weighted(
            [filter_taps[z + 8 - 4 * offset] for z in planes], [deep[z][sy] for z in planes]
        )

    offsets = (2, -2, -3, 1, -1)
    for index, offset in enumerate(offsets):
        for sz in range(2):
            for sy in range(2):
                part_out[index, sz, sy] = partial(sz, sy, offset)

    @pl.when(gy == 0)
    def _():
        pl.semaphore_wait(barrier, 16)
        signal(link, other_core)

    @pl.when(gy == 1)
    def _():
        pl.semaphore_wait(link, 1)

    part_copies = send_all(
        part_in,
        *(
            (part_out.at[index], part_in.at[index], along(offset))
            for index, offset in enumerate(offsets)
        ),
    )

    for z in range(4):
        for sx in range(2):
            taps = [xa[sx, z, pl.ds(j, 16, stride=2), :] for j in range(8)]
            zw[6 + z, sx] = weighted(LOWPASS, taps)
            zw[6 + z, 2 + sx] = weighted(HIGHPASS, taps)
    six = zw.at[0:6]
    plane_copies = send_all(
        six,
        (zw.at[6:10, 0:2], zw.at[2:6, 0:2], along(1)),
        (zw.at[6:10, 2:4], zw.at[10:14, 2:4], along(-1)),
        (zw.at[8:10, 2:4], zw.at[4:6, 2:4], along(1)),
        (zw.at[6:8, 0:2], zw.at[10:12, 0:2], along(-1)),
    )
    @pl.when(gy == 0)
    def _():
        signal(near, along(3), along(-3), across_x(1, gy), across_x(-1, gy))

    plane_copies.wait_send()
    more_copies = send_all(
        six,
        (zw.at[8:10], zw.at[0:2], along(2)),
        (zw.at[6:8], zw.at[14:16], along(-2)),
        (zw.at[6:8, 2:4], zw.at[2:4, 2:4], along(1)),
        (zw.at[8:10, 0:2], zw.at[12:14, 0:2], along(-1)),
    )

    lane = lax.broadcasted_iota(jnp.int32, (8, 128), 1)
    first_half = lane < 64
    zero = jnp.zeros((8, 128), jnp.float32)
    loads[2].wait()
    limits = [thr[t] for t in range(4)]
    squares = [limit * limit for limit in limits]

    part_copies.wait_recv()

    @pl.when(gy == 0)
    def _():
        pl.semaphore_wait(near, 4)
        signal(mid, along(2), along(-2), across_x(2, gy), across_x(-2, gy))

    residual = [zero] * 4
    weight = [zero] * 4
    for sz in range(2):
        for sy in range(2):
            c = partial(sz, sy, 0)
            for index in range(5):
                c = c + part_in[index, sz, sy]
            cb[3, sz, sy, 8:16, :] = c
    coeff_copies = send_all(
        cb.at[0:5, :, :, 8:16, :],
        *(
            (cb.at[3, :, :, 8:16, :], cb.at[3 - offset, :, :, 8:16, :], along(offset))
            for offset in (3, -2, 2, -1, 1)
        ),
    )
    for sz in range(2):
        for sy in range(2):
            c = cb[3, sz, sy, 8:16, :]
            square = c * c
            for t in range(4):
                cut = jnp.clip(c, -limits[t], limits[t])
                kept = squares[t] / (squares[t] + square)
                cut = cut * cut
                if sz == 0 and sy == 0:
                    cut = jnp.where(first_half, zero, cut)
                    kept = jnp.where(first_half, zero, kept)
                residual[t] = residual[t] + cut
                weight[t] = weight[t] + kept

    def level_one(k, half):
        for sx in range(2):
            band = 2 * half + sx
            planes = [zw[2 * k + j, band] for j in range(8)]
            if band:
                db[k, 2 * band - 1, 8:24, :] = weighted(LOWPASS, planes)
            db[k, 2 * band, 8:24, :] = weighted(HIGHPASS, planes)

    plane_copies.wait_recv()

    @pl.when(gy == 0)
    def _():
        pl.semaphore_wait(mid, 4)
        signal(link, other_core)

    for k in range(2):
        level_one(1 + k, 0)
        level_one(2 + k, 1)

    def add_bands(first):
        def add_band(band, sums):
            sums = list(sums)
            for k in range(2):
                for half in range(2):
                    c = db[first + k, band, 8 + 8 * half : 16 + 8 * half, :]
                    square = c * c
                    for t in range(4):
                        cut = jnp.clip(c, -limits[t], limits[t])
                        sums[t] = sums[t] + cut * cut
                        sums[4 + t] = sums[4 + t] + squares[t] / (squares[t] + square)
            return tuple(sums)

        return add_band

    sums = lax.fori_loop(0, 3, add_bands(1), tuple(residual + weight))
    sums = lax.fori_loop(3, 7, add_bands(2), sums)

    def as_row(parts):
        line = jnp.zeros((1, 128), jnp.float32)
        for t, part in enumerate(parts):
            value = jnp.sum(jnp.sum(part, axis=0, keepdims=True), axis=1, keepdims=True)
            line = jnp.where(lane[0:1] == t, value, line)
        return line

    row[0:1, :] = as_row(sums[0:4])
    row[1:2, :] = as_row(sums[4:8])
    slot = gy * nx + gx
    arx[pl.ds(slot, 1)] = row[...].reshape(1, 2, 128)

    @pl.when(gy == 1)
    def _():
        pl.semaphore_wait(link, 1)

    x_copies = send_all(
        arx.at[0 : 2 * nx - 1],
        *(
            (row, arx.at[slot], across_x(offset, place))
            for offset in sorted(range(nx), key=lambda o: -min(o, nx - o))
            for place in (gy, other)
            if not (place is gy and offset == 0)
        ),
    )

    more_copies.wait_recv()
    for k in range(5):
        for half in range(2):
            if k - half not in (1, 2):
                level_one(k, half)

    detail_rows = send_all(
        db.at[:, :, 16:24, :], (db.at[:, :, 16:24, :], db.at[:, :, 0:8, :], other_core)
    )
    detail_rows.wait_recv()

    def along_z(t, carry):
        limit = thr[t]
        for part in range(3):
            rows = slice(8 * part, 8 * part + 8)

            def cut(band):
                return [shrunk(db[k, band, rows, :], limit) for k in range(5)]

            pairs = ((None, cut(0)), (cut(1), cut(2)), (cut(3), cut(4)), (cut(5), cut(6)))
            for band, (low, high) in enumerate(pairs):
                for e in range(2):
                    order = [3 + e - i for i in range(4)]
                    for odd in range(2):
                        value = weighted(HIGHPASS[odd::2], [high[i] for i in order])
                        if low is not None:
                            value = value + weighted(LOWPASS[odd::2], [low[i] for i in order])
                        zs1[2 * e + odd, t, band, rows, :] = value
        return carry

    lax.fori_loop(0, 4, along_z, 0)

    coeff_copies.wait_recv()
    deep_rows = send_all(
        cb.at[:, :, :, 8:16, :],
        (cb.at[:, :, :, 8:16, :], cb.at[:, :, :, 0:8, :], other_core),
    )

    x_copies.wait_recv()
    tot[...] = jnp.sum(arx[...], axis=0)
    arz[pl.ds(gz, 1)] = tot[...].reshape(1, 2, 128)
    z_copies = send_all(
        arz.at[0 : nz - 1],
        *(
            (tot, arz.at[gz], across_z(offset))
            for offset in sorted(range(1, nz), key=lambda o: min(o, nz - o))
        ),
    )

    deep_rows.wait_recv()

    def deep_along_z(t, carry):
        limit = thr[t]
        for sy in range(2):
            for part in range(2):
                bands = []
                for sz in range(2):
                    values = []
                    for m in range(6):
                        c = cb[m, sz, sy, 8 * part : 8 * part + 8, :]
                        s = shrunk(c, limit)
                        values.append(jnp.where(first_half, c, s) if sz + sy == 0 else s)
                    bands.append(values)
                for k in range(5):
                    p = 3 + (k + 1) // 2
                    odd = (k + 1) % 2
                    order = [p - i for i in range(4)]
                    zs2[t, k, sy, 8 + 8 * part : 16 + 8 * part, :] = synthesis_pair(
                        [bands[0][i] for i in order], [bands[1][i] for i in order], odd
                    )
        return carry

    lax.fori_loop(0, 4, deep_along_z, 0)

    def deep_along_y(t, carry):
        for k in range(5):
            low = [zs2[t, k, 0, 8 - i : 24 - i, :] for i in range(4)]
            high = [zs2[t, k, 1, 8 - i : 24 - i, :] for i in range(4)]
            co[t, k, pl.ds(0, 16, stride=2), :] = synthesis_pair(low, high, 0)
            co[t, k, pl.ds(1, 16, stride=2), :] = synthesis_pair(low, high, 1)
        return carry

    lax.fori_loop(0, 4, deep_along_y, 0)
    loads[3].wait()
    cr[...] = product(co[:, :, 8:32, :].reshape(480, 128), a2t).reshape(4, 5, 24, 128)

    def along_y(t, carry):
        for part in range(3):
            rows = slice(8 * part, 8 * part + 8)
            low = [cr[t, k, rows, :] for k in range(5)]
            for e in range(2):
                order = [3 + e - i for i in range(4)]
                for odd in range(2):
                    zs1[2 * e + odd, t, 0, rows, :] = zs1[
                        2 * e + odd, t, 0, rows, :
                    ] + weighted(LOWPASS[odd::2], [low[i] for i in order])
        for z in range(4):
            for sx in range(2):
                low = [zs1[z, t, sx, 8 - i : 24 - i, :] for i in range(4)]
                high = [zs1[z, t, 2 + sx, 8 - i : 24 - i, :] for i in range(4)]
                fo[sx, z, t, pl.ds(0, 16, stride=2), :] = synthesis_pair(low, high, 0)
                fo[sx, z, t, pl.ds(1, 16, stride=2), :] = synthesis_pair(low, high, 1)
        return carry

    lax.fori_loop(0, 4, along_y, 0)
    loads[4].wait()
    both = jnp.concatenate([fo[0].reshape(512, 128), fo[1].reshape(512, 128)], axis=1)
    den[...] = product(both, a1t).reshape(4, 4, 32, 256)

    z_copies.wait_recv()
    full = jnp.sum(arz[...], axis=0)
    cells = float(4 * 32 * 256 * total * 2)
    weights = jnp.where(lane[0:1] < 4, full[1:2], 1.0)
    gcv[...] = (cells * full[0:1] / (weights * weights))[:, 0:4]
    for group in groups:
        if group is not plane_copies:
            group.wait_send()


def solution(mesh):
    nx, nz = 8, 16
    return on_grid(mesh, nx, nz)


def on_grid(mesh, nx, nz):
    split = Mesh(
        mesh.devices.reshape(mesh.shape["cube"], nx, nz, mesh.shape["gy"]),
        ("cube", "gz_0", "gz_1", "gy"),
    )
    first = analysis_matrix(256)
    second = analysis_matrix(128)
    forward = np.concatenate([first, first[:, 0:128] @ second], axis=1)
    matrices = [in_two_parts(m) for m in (forward, first.T, second.T)]
    f32 = jnp.float32

    def body(noisy_cube, thresholds):
        den, gcv = pl.pallas_call(
            functools.partial(kernel, nx, nz),
            out_shape=(
                jax.ShapeDtypeStruct((4, 4, 32, 256), f32),
                jax.ShapeDtypeStruct((1, 4), f32),
            ),
            in_specs=[pl.BlockSpec(memory_space=pltpu.HBM)] * 5,
            out_specs=(
                pl.BlockSpec(memory_space=pltpu.VMEM),
                pl.BlockSpec(memory_space=pltpu.VMEM),
            ),
            scratch_shapes=[
                pltpu.SMEM((4,), f32),
                pltpu.VMEM((4, 56, 256), f32),
                pltpu.VMEM((3, 4, 56, 128), f32),
                pltpu.VMEM((16, 4, 16, 128), f32),
                pltpu.VMEM((5, 2, 2, 8, 128), f32),
                pltpu.VMEM((5, 2, 2, 8, 128), f32),
                pltpu.VMEM((5, 7, 24, 128), f32),
                pltpu.VMEM((6, 2, 2, 16, 128), f32),
                pltpu.VMEM((4, 5, 2, 24, 128), f32),
                pltpu.VMEM((4, 5, 32, 128), f32),
                pltpu.VMEM((4, 5, 24, 128), f32),
                pltpu.VMEM((4, 4, 4, 24, 128), f32),
                pltpu.VMEM((2, 4, 4, 32, 128), f32),
                pltpu.VMEM((2, 256, 384), jnp.bfloat16),
                pltpu.VMEM((2, 256, 256), jnp.bfloat16),
                pltpu.VMEM((2, 128, 128), jnp.bfloat16),
                pltpu.VMEM((2, 128), f32),
                pltpu.VMEM((2, 128), f32),
                pltpu.VMEM((2 * nx, 2, 128), f32),
                pltpu.VMEM((nz, 2, 128), f32),
                pltpu.SemaphoreType.DMA((5,)),
                pltpu.SemaphoreType.DMA((9,)),
                pltpu.SemaphoreType.DMA((9,)),
                pltpu.SemaphoreType.REGULAR,
                pltpu.SemaphoreType.REGULAR,
                pltpu.SemaphoreType.REGULAR,
            ],
            compiler_params=pltpu.CompilerParams(
                collective_id=0, has_side_effects=True, vmem_limit_bytes=12 * 1024 * 1024
            ),
        )(*(pltpu.with_memory_space_constraint(v, pltpu.HBM) for v in (thresholds, noisy_cube, *(jnp.asarray(m) for m in matrices))))
        return den, gcv.reshape(4)

    return jax.shard_map(
        body,
        mesh=split,
        in_specs=(P(CUBE_GZ, "gy", None), P()),
        out_specs=(P(CUBE_GZ, None, "gy", None), P("cube")),
        check_vma=False,
    )
```

```python
import functools

import jax
import jax.numpy as jnp
import numpy as np
from jax import lax
from jax.experimental import pallas as pl
from jax.experimental.pallas import tpu as pltpu
from jax.sharding import Mesh
from jax.sharding import PartitionSpec as P

MESH = pl.DeviceIdType.MESH
CUBE_GZ = ("cube", "gz_0", "gz_1")

LOWPASS = (
    0.2303778133088964,
    0.7148465705529155,
    0.6308807679298587,
    -0.0279837694168599,
    -0.1870348117190931,
    0.0308413818355607,
    0.0328830116668852,
    -0.010597401785069,
)
HIGHPASS = tuple(((-1) ** tap * LOWPASS[7 - tap] for tap in range(8)))


def composed(second):
    taps = np.zeros(22)
    for outer in range(8):
        for inner in range(8):
            taps[2 * outer + inner] += second[outer] * LOWPASS[inner]
    return tuple(float(tap) for tap in taps)


DEEP_LOW = composed(LOWPASS)
DEEP_HIGH = composed(HIGHPASS)


def analysis_matrix(length):
    matrix = np.zeros((length, length))
    for k in range(length // 2):
        for tap in range(8):
            matrix[(2 * k + tap) % length, k] += LOWPASS[tap]
            matrix[(2 * k + tap) % length, length // 2 + k] += HIGHPASS[tap]
    return matrix


def in_two_parts(matrix):
    exact = matrix.astype(np.float32)
    upper = exact.astype(jnp.bfloat16)
    lower = (exact - upper.astype(np.float32)).astype(jnp.bfloat16)
    return np.stack([upper, lower])


def product(values, parts):
    upper = values.astype(jnp.bfloat16)
    lower = (values - upper.astype(jnp.float32)).astype(jnp.bfloat16)
    dot = functools.partial(jnp.dot, preferred_element_type=jnp.float32)
    return dot(upper, parts[0]) + (dot(lower, parts[0]) + dot(upper, parts[1]))


def weighted(taps, values):
    result = taps[0] * values[0]
    for tap, value in zip(taps[1:], values[1:]):
        result = result + tap * value
    return result


def synthesis_pair(low, high, odd):
    return weighted(LOWPASS[odd::2], low) + weighted(HIGHPASS[odd::2], high)


def shrunk(values, limit):
    return values - jnp.clip(values, -limit, limit)


def kernel(
    nx,
    nz,
    thr_hbm,
    x_hbm,
    a1_hbm,
    a1t_hbm,
    a2t_hbm,
    den,
    gcv,
    thr,
    raw,
    xa,
    zw,
    part_out,
    part_in,
    db,
    cb,
    zs2,
    co,
    cr,
    zs1,
    fo,
    a1,
    a1t,
    a2t,
    row,
    tot,
    arx,
    arz,
    local_sem,
    send_sem,
    recv_sem,
    link,
    near_x,
    mid_x,
    near_z,
    mid_z,
):
    cube, gx, gz, gy = (lax.axis_index(n) for n in ("cube", "gz_0", "gz_1", "gy"))
    total = nx * nz
    flat = gx * nz + gz
    other = 1 - gy
    other_core = (cube, gx, gz, other)

    def along(offset, core=None):
        place = lax.rem(flat + (offset + total), total)
        return (cube, lax.div(place, nz), lax.rem(place, nz), gy if core is None else core)

    def across_x(offset, core):
        return (cube, lax.rem(gx + (offset + nx), nx), gz, core)

    def across_z(offset):
        return (cube, gx, lax.rem(gz + (offset + 2 * nz), nz), gy)

    groups = []

    def send_all(whole, *copies):
        index = len(groups)
        sems = (send_sem.at[index], recv_sem.at[index])
        for src, dst, device in copies:
            pltpu.make_async_remote_copy(
                src_ref=src,
                dst_ref=dst,
                send_sem=sems[0],
                recv_sem=sems[1],
                device_id=device,
                device_id_type=MESH,
            ).start()
        group = pltpu.make_async_remote_copy(
            src_ref=whole,
            dst_ref=whole,
            send_sem=sems[0],
            recv_sem=sems[1],
            device_id=other_core,
            device_id_type=MESH,
        )
        groups.append(group)
        return group

    def signal(sem, *devices):
        for device in devices:
            pl.semaphore_signal(sem, inc=1, device_id=device, device_id_type=MESH)

    loads = [pltpu.make_async_copy(x_hbm, raw.at[:, 0:32, :], local_sem.at[0])]
    for index, (src, dst) in enumerate(
        ((a1_hbm, a1), (thr_hbm, thr), (a2t_hbm, a2t), (a1t_hbm, a1t))
    ):
        loads.append(pltpu.make_async_copy(src, dst, local_sem.at[index + 1]))
    for load in loads:
        load.start()

    barrier = pltpu.get_barrier_semaphore()

    @pl.when(gy == 0)
    def _():
        signal(barrier, other_core)

    around = [along(offset, 0) for offset in (3, -3, 2, -2, 1, -1)]
    signal(barrier, *around, across_x(1, 0), across_x(-1, 0))

    @pl.when(gy == 1)
    def _():
        pl.semaphore_wait(barrier, 1)
        signal(link, other_core)

    @pl.when(gy == 0)
    def _():
        pl.semaphore_wait(link, 1)

    loads[0].wait()
    rows_copy = send_all(
        raw.at[:, 0:24, :], (raw.at[:, 0:24, :], raw.at[:, 32:56, :], other_core)
    )

    loads[1].wait()
    own = product(raw[:, 0:32, :].reshape(128, 256), a1)
    for band in range(3):
        xa[band, :, 0:32, :] = own[:, 128 * band : 128 * band + 128].reshape(4, 32, 128)
    rows_copy.wait_recv()
    beyond = product(raw[:, 32:56, :].reshape(96, 256), a1)
    for band in range(3):
        xa[band, :, 32:56, :] = beyond[:, 128 * band : 128 * band + 128].reshape(4, 24, 128)

    deep = []
    for z in range(4):
        taps = [xa[2, z, pl.ds(i, 8, stride=4), :] for i in range(22)]
        deep.append((weighted(DEEP_LOW, taps), weighted(DEEP_HIGH, taps)))

    def partial(sz, sy, offset):
        filter_taps = (DEEP_LOW, DEEP_HIGH)[sz]
        planes = [z for z in range(4) if z + 8 - 4 * offset < 22]
        return weighted(
            [filter_taps[z + 8 - 4 * offset] for z in planes], [deep[z][sy] for z in planes]
        )

    offsets = (2, -2, -3, 1, -1)
    for index, offset in enumerate(offsets):
        for sz in range(2):
            for sy in range(2):
                part_out[index, sz, sy] = partial(sz, sy, offset)

    @pl.when(gy == 0)
    def _():
        pl.semaphore_wait(barrier, 16)
        signal(link, other_core)

    @pl.when(gy == 1)
    def _():
        pl.semaphore_wait(link, 1)

    part_copies = send_all(
        part_in,
        *(
            (part_out.at[index], part_in.at[index], along(offset))
            for index, offset in enumerate(offsets)
        ),
    )

    for z in range(4):
        for sx in range(2):
            taps = [xa[sx, z, pl.ds(j, 16, stride=2), :] for j in range(8)]
            zw[6 + z, sx] = weighted(LOWPASS, taps)
            zw[6 + z, 2 + sx] = weighted(HIGHPASS, taps)
    plane_copies = send_all(
        zw.at[0:6],
        (zw.at[6:10, 0:2], zw.at[2:6, 0:2], along(1)),
        (zw.at[6:10, 2:4], zw.at[10:14, 2:4], along(-1)),
        (zw.at[8:10, 2:4], zw.at[4:6, 2:4], along(1)),
        (zw.at[6:8, 0:2], zw.at[10:12, 0:2], along(-1)),
    )

    @pl.when(gy == 0)
    def _():
        signal(near_x, across_x(1, gy), across_x(-1, gy))

    @pl.when(gy == 0)
    def _():
        pl.semaphore_wait(near_x, 2)
        signal(mid_x, across_x(2, gy), across_x(-2, gy))

    lane = lax.broadcasted_iota(jnp.int32, (8, 128), 1)
    first_half = lane < 64
    zero = jnp.zeros((8, 128), jnp.float32)
    loads[2].wait()
    limits = [thr[t] for t in range(4)]
    squares = [limit * limit for limit in limits]

    part_copies.wait_recv()
    residual = [zero] * 4
    weight = [zero] * 4
    for sz in range(2):
        for sy in range(2):
            c = partial(sz, sy, 0)
            for index in range(5):
                c = c + part_in[index, sz, sy]
            cb[3, sz, sy, 8:16, :] = c
    coeff_copies = send_all(
        cb.at[0:5, :, :, 8:16, :],
        *(
            (cb.at[3, :, :, 8:16, :], cb.at[3 - offset, :, :, 8:16, :], along(offset))
            for offset in (3, -2, 2, -1, 1)
        ),
    )
    for sz in range(2):
        for sy in range(2):
            c = cb[3, sz, sy, 8:16, :]
            square = c * c
            for t in range(4):
                cut = jnp.clip(c, -limits[t], limits[t])
                kept = squares[t] / (squares[t] + square)
                cut = cut * cut
                if sz == 0 and sy == 0:
                    cut = jnp.where(first_half, zero, cut)
                    kept = jnp.where(first_half, zero, kept)
                residual[t] = residual[t] + cut
                weight[t] = weight[t] + kept

    def level_one(k, half):
        for sx in range(2):
            band = 2 * half + sx
            planes = [zw[2 * k + j, band] for j in range(8)]
            if band:
                db[k, 2 * band - 1, 8:24, :] = weighted(LOWPASS, planes)
            db[k, 2 * band, 8:24, :] = weighted(HIGHPASS, planes)

    @pl.when(gy == 0)
    def _():
        pl.semaphore_wait(mid_x, 2)
        signal(link, other_core)
        signal(near_z, across_z(3), across_z(-3))

    plane_copies.wait_recv()
    for k in range(2):
        level_one(1 + k, 0)
        level_one(2 + k, 1)

    def add_bands(first):
        def add_band(band, sums):
            sums = list(sums)
            for k in range(2):
                for half in range(2):
                    c = db[first + k, band, 8 + 8 * half : 16 + 8 * half, :]
                    square = c * c
                    for t in range(4):
                        cut = jnp.clip(c, -limits[t], limits[t])
                        sums[t] = sums[t] + cut * cut
                        sums[4 + t] = sums[4 + t] + squares[t] / (squares[t] + square)
            return tuple(sums)

        return add_band

    sums = lax.fori_loop(0, 3, add_bands(1), tuple(residual + weight))
    sums = lax.fori_loop(3, 7, add_bands(2), sums)

    def as_row(parts):
        line = jnp.zeros((1, 128), jnp.float32)
        for t, part in enumerate(parts):
            value = jnp.sum(jnp.sum(part, axis=0, keepdims=True), axis=1, keepdims=True)
            line = jnp.where(lane[0:1] == t, value, line)
        return line

    row[0:1, :] = as_row(sums[0:4])
    row[1:2, :] = as_row(sums[4:8])
    slot = gy * nx + gx
    arx[pl.ds(slot, 1)] = row[...].reshape(1, 2, 128)

    @pl.when(gy == 1)
    def _():
        pl.semaphore_wait(link, 1)

    x_copies = send_all(
        arx.at[0 : 2 * nx - 1],
        *(
            (row, arx.at[slot], across_x(offset, place))
            for offset in sorted(range(nx), key=lambda o: -min(o, nx - o))
            for place in (gy, other)
            if not (place is gy and offset == 0)
        ),
    )

    detail_copies = send_all(
        db.at[0:3, :, 8:24, :],
        (db.at[2:4, 3:7, 8:24, :], db.at[0:2, 3:7, 8:24, :], along(1)),
        (db.at[1:3, 0:3, 8:24, :], db.at[3:5, 0:3, 8:24, :], along(-1)),
        (db.at[2, 0:3, 8:24, :], db.at[0, 0:3, 8:24, :], along(1)),
        (db.at[2, 3:7, 8:24, :], db.at[4, 3:7, 8:24, :], along(-1)),
    )

    @pl.when(gy == 0)
    def _():
        pl.semaphore_wait(near_z, 2)
        signal(mid_z, across_z(2), across_z(-2))

    @pl.when(gy == 0)
    def _():
        pl.semaphore_wait(mid_z, 2)
        signal(link, other_core)

    x_copies.wait_recv()

    @pl.when(gy == 1)
    def _():
        pl.semaphore_wait(link, 1)

    tot[...] = jnp.sum(arx[...], axis=0)
    arz[pl.ds(gz, 1)] = tot[...].reshape(1, 2, 128)
    z_copies = send_all(
        arz.at[0 : nz - 1],
        *(
            (tot, arz.at[gz], across_z(offset))
            for offset in sorted(range(1, nz), key=lambda o: min(o, nz - o))
        ),
    )

    coeff_copies.wait_recv()
    deep_rows = send_all(
        cb.at[:, :, :, 8:16, :],
        (cb.at[:, :, :, 8:16, :], cb.at[:, :, :, 0:8, :], other_core),
    )

    detail_copies.wait_recv()
    detail_rows = send_all(
        db.at[:, :, 16:24, :], (db.at[:, :, 16:24, :], db.at[:, :, 0:8, :], other_core)
    )

    deep_rows.wait_recv()

    def deep_along_z(t, carry):
        limit = thr[t]
        for sy in range(2):
            for part in range(2):
                bands = []
                for sz in range(2):
                    values = []
                    for m in range(6):
                        c = cb[m, sz, sy, 8 * part : 8 * part + 8, :]
                        s = shrunk(c, limit)
                        values.append(jnp.where(first_half, c, s) if sz + sy == 0 else s)
                    bands.append(values)
                for k in range(5):
                    p = 3 + (k + 1) // 2
                    odd = (k + 1) % 2
                    order = [p - i for i in range(4)]
                    zs2[t, k, sy, 8 + 8 * part : 16 + 8 * part, :] = synthesis_pair(
                        [bands[0][i] for i in order], [bands[1][i] for i in order], odd
                    )
        return carry

    lax.fori_loop(0, 4, deep_along_z, 0)

    def deep_along_y(t, carry):
        for k in range(5):
            low = [zs2[t, k, 0, 8 - i : 24 - i, :] for i in range(4)]
            high = [zs2[t, k, 1, 8 - i : 24 - i, :] for i in range(4)]
            co[t, k, pl.ds(0, 16, stride=2), :] = synthesis_pair(low, high, 0)
            co[t, k, pl.ds(1, 16, stride=2), :] = synthesis_pair(low, high, 1)
        return carry

    lax.fori_loop(0, 4, deep_along_y, 0)
    loads[3].wait()
    cr[...] = product(co[:, :, 8:32, :].reshape(480, 128), a2t).reshape(4, 5, 24, 128)

    detail_rows.wait_recv()

    def along_z(t, carry):
        limit = thr[t]
        for part in range(3):
            rows = slice(8 * part, 8 * part + 8)

            def cut(band):
                return [shrunk(db[k, band, rows, :], limit) for k in range(5)]

            pairs = ((None, cut(0)), (cut(1), cut(2)), (cut(3), cut(4)), (cut(5), cut(6)))
            for band, (low, high) in enumerate(pairs):
                for e in range(2):
                    order = [3 + e - i for i in range(4)]
                    for odd in range(2):
                        value = weighted(HIGHPASS[odd::2], [high[i] for i in order])
                        if low is not None:
                            value = value + weighted(LOWPASS[odd::2], [low[i] for i in order])
                        zs1[2 * e + odd, t, band, rows, :] = value
        return carry

    lax.fori_loop(0, 4, along_z, 0)

    def along_y(t, carry):
        for part in range(3):
            rows = slice(8 * part, 8 * part + 8)
            low = [cr[t, k, rows, :] for k in range(5)]
            for e in range(2):
                order = [3 + e - i for i in range(4)]
                for odd in range(2):
                    zs1[2 * e + odd, t, 0, rows, :] = zs1[
                        2 * e + odd, t, 0, rows, :
                    ] + weighted(LOWPASS[odd::2], [low[i] for i in order])
        for z in range(4):
            for sx in range(2):
                low = [zs1[z, t, sx, 8 - i : 24 - i, :] for i in range(4)]
                high = [zs1[z, t, 2 + sx, 8 - i : 24 - i, :] for i in range(4)]
                fo[sx, z, t, pl.ds(0, 16, stride=2), :] = synthesis_pair(low, high, 0)
                fo[sx, z, t, pl.ds(1, 16, stride=2), :] = synthesis_pair(low, high, 1)
        return carry

    lax.fori_loop(0, 4, along_y, 0)
    loads[4].wait()
    both = jnp.concatenate([fo[0].reshape(512, 128), fo[1].reshape(512, 128)], axis=1)
    den[...] = product(both, a1t).reshape(4, 4, 32, 256)

    z_copies.wait_recv()
    full = jnp.sum(arz[...], axis=0)
    cells = float(4 * 32 * 256 * total * 2)
    weights = jnp.where(lane[0:1] < 4, full[1:2], 1.0)
    gcv[...] = (cells * full[0:1] / (weights * weights))[:, 0:4]
    for group in groups:
        group.wait_send()


def solution(mesh):
    nx, nz = 8, 16
    return on_grid(mesh, nx, nz)


def on_grid(mesh, nx, nz):
    split = Mesh(
        mesh.devices.reshape(mesh.shape["cube"], nx, nz, mesh.shape["gy"]),
        ("cube", "gz_0", "gz_1", "gy"),
    )
    first = analysis_matrix(256)
    second = analysis_matrix(128)
    forward = np.concatenate([first, first[:, 0:128] @ second], axis=1)
    matrices = [in_two_parts(m) for m in (forward, first.T, second.T)]
    f32 = jnp.float32

    def body(noisy_cube, thresholds):
        den, gcv = pl.pallas_call(
            functools.partial(kernel, nx, nz),
            out_shape=(
                jax.ShapeDtypeStruct((4, 4, 32, 256), f32),
                jax.ShapeDtypeStruct((1, 4), f32),
            ),
            in_specs=[pl.BlockSpec(memory_space=pltpu.HBM)] * 5,
            out_specs=(
                pl.BlockSpec(memory_space=pltpu.VMEM),
                pl.BlockSpec(memory_space=pltpu.VMEM),
            ),
            scratch_shapes=[
                pltpu.SMEM((4,), f32),
                pltpu.VMEM((4, 56, 256), f32),
                pltpu.VMEM((3, 4, 56, 128), f32),
                pltpu.VMEM((16, 4, 16, 128), f32),
                pltpu.VMEM((5, 2, 2, 8, 128), f32),
                pltpu.VMEM((5, 2, 2, 8, 128), f32),
                pltpu.VMEM((5, 7, 24, 128), f32),
                pltpu.VMEM((6, 2, 2, 16, 128), f32),
                pltpu.VMEM((4, 5, 2, 24, 128), f32),
                pltpu.VMEM((4, 5, 32, 128), f32),
                pltpu.VMEM((4, 5, 24, 128), f32),
                pltpu.VMEM((4, 4, 4, 24, 128), f32),
                pltpu.VMEM((2, 4, 4, 32, 128), f32),
                pltpu.VMEM((2, 256, 384), jnp.bfloat16),
                pltpu.VMEM((2, 256, 256), jnp.bfloat16),
                pltpu.VMEM((2, 128, 128), jnp.bfloat16),
                pltpu.VMEM((2, 128), f32),
                pltpu.VMEM((2, 128), f32),
                pltpu.VMEM((2 * nx, 2, 128), f32),
                pltpu.VMEM((nz, 2, 128), f32),
                pltpu.SemaphoreType.DMA((5,)),
                pltpu.SemaphoreType.DMA((9,)),
                pltpu.SemaphoreType.DMA((9,)),
                pltpu.SemaphoreType.REGULAR,
                pltpu.SemaphoreType.REGULAR,
                pltpu.SemaphoreType.REGULAR,
                pltpu.SemaphoreType.REGULAR,
                pltpu.SemaphoreType.REGULAR,
            ],
            compiler_params=pltpu.CompilerParams(
                collective_id=0, has_side_effects=True, vmem_limit_bytes=12 * 1024 * 1024
            ),
        )(*(pltpu.with_memory_space_constraint(v, pltpu.HBM) for v in (thresholds, noisy_cube, *(jnp.asarray(m) for m in matrices))))
        return den, gcv.reshape(4)

    return jax.shard_map(
        body,
        mesh=split,
        in_specs=(P(CUBE_GZ, "gy", None), P()),
        out_specs=(P(CUBE_GZ, None, "gy", None), P("cube")),
        check_vma=False,
    )
```

```python
import functools

import jax
import jax.numpy as jnp
import numpy as np
from jax import lax
from jax.experimental import pallas as pl
from jax.experimental.pallas import tpu as pltpu
from jax.sharding import Mesh
from jax.sharding import PartitionSpec as P

MESH = pl.DeviceIdType.MESH
CUBE_GZ = ("cube", "gz_0", "gz_1")

LOWPASS = (
    0.2303778133088964,
    0.7148465705529155,
    0.6308807679298587,
    -0.0279837694168599,
    -0.1870348117190931,
    0.0308413818355607,
    0.0328830116668852,
    -0.010597401785069,
)
HIGHPASS = tuple(((-1) ** tap * LOWPASS[7 - tap] for tap in range(8)))


def composed(second):
    taps = np.zeros(22)
    for outer in range(8):
        for inner in range(8):
            taps[2 * outer + inner] += second[outer] * LOWPASS[inner]
    return tuple(float(tap) for tap in taps)


DEEP_LOW = composed(LOWPASS)
DEEP_HIGH = composed(HIGHPASS)


def analysis_matrix(length):
    matrix = np.zeros((length, length))
    for k in range(length // 2):
        for tap in range(8):
            matrix[(2 * k + tap) % length, k] += LOWPASS[tap]
            matrix[(2 * k + tap) % length, length // 2 + k] += HIGHPASS[tap]
    return matrix


def in_two_parts(matrix):
    exact = matrix.astype(np.float32)
    upper = exact.astype(jnp.bfloat16)
    lower = (exact - upper.astype(np.float32)).astype(jnp.bfloat16)
    return np.stack([upper, lower])


def product(values, parts):
    upper = values.astype(jnp.bfloat16)
    lower = (values - upper.astype(jnp.float32)).astype(jnp.bfloat16)
    dot = functools.partial(jnp.dot, preferred_element_type=jnp.float32)
    return dot(upper, parts[0]) + (dot(lower, parts[0]) + dot(upper, parts[1]))


def weighted(taps, values):
    result = taps[0] * values[0]
    for tap, value in zip(taps[1:], values[1:]):
        result = result + tap * value
    return result


def synthesis_pair(low, high, odd):
    return weighted(LOWPASS[odd::2], low) + weighted(HIGHPASS[odd::2], high)


def shrunk(values, limit):
    return values - jnp.clip(values, -limit, limit)


def kernel(
    nx,
    nz,
    thr_hbm,
    x_hbm,
    a1_hbm,
    a1t_hbm,
    a2t_hbm,
    den,
    gcv,
    thr,
    raw,
    xa,
    zw,
    part_out,
    part_in,
    db,
    cb,
    zs2,
    co,
    cr,
    zs1,
    fo,
    a1,
    a1t,
    a2t,
    row,
    tot,
    arx,
    arz,
    local_sem,
    send_sem,
    recv_sem,
    link,
    near_x,
    mid_x,
    near_z,
    mid_z,
):
    cube, gx, gz, gy = (lax.axis_index(n) for n in ("cube", "gz_0", "gz_1", "gy"))
    total = nx * nz
    flat = gx * nz + gz
    other = 1 - gy
    other_core = (cube, gx, gz, other)

    def along(offset, core=None):
        place = lax.rem(flat + (offset + total), total)
        return (cube, lax.div(place, nz), lax.rem(place, nz), gy if core is None else core)

    def across_x(offset, core):
        return (cube, lax.rem(gx + (offset + nx), nx), gz, core)

    def across_z(offset):
        return (cube, gx, lax.rem(gz + (offset + 2 * nz), nz), gy)

    groups = []

    def send_all(whole, *copies):
        index = len(groups)
        sems = (send_sem.at[index], recv_sem.at[index])
        for src, dst, device in copies:
            pltpu.make_async_remote_copy(
                src_ref=src,
                dst_ref=dst,
                send_sem=sems[0],
                recv_sem=sems[1],
                device_id=device,
                device_id_type=MESH,
            ).start()
        group = pltpu.make_async_remote_copy(
            src_ref=whole,
            dst_ref=whole,
            send_sem=sems[0],
            recv_sem=sems[1],
            device_id=other_core,
            device_id_type=MESH,
        )
        groups.append(group)
        return group

    def signal(sem, *devices):
        for device in devices:
            pl.semaphore_signal(sem, inc=1, device_id=device, device_id_type=MESH)

    loads = [pltpu.make_async_copy(x_hbm, raw.at[:, 0:32, :], local_sem.at[0])]
    for index, (src, dst) in enumerate(
        ((a1_hbm, a1), (thr_hbm, thr), (a2t_hbm, a2t), (a1t_hbm, a1t))
    ):
        loads.append(pltpu.make_async_copy(src, dst, local_sem.at[index + 1]))
    for load in loads:
        load.start()

    barrier = pltpu.get_barrier_semaphore()

    @pl.when(gy == 0)
    def _():
        signal(barrier, other_core)

    around = [along(offset, 0) for offset in (3, -3, 2, -2, 1, -1)]
    signal(barrier, *around, across_x(1, 0), across_x(-1, 0))

    @pl.when(gy == 1)
    def _():
        pl.semaphore_wait(barrier, 1)
        signal(link, other_core)

    @pl.when(gy == 0)
    def _():
        pl.semaphore_wait(link, 1)

    loads[0].wait()
    rows_copy = send_all(
        raw.at[:, 0:24, :], (raw.at[:, 0:24, :], raw.at[:, 32:56, :], other_core)
    )

    loads[1].wait()
    own = product(raw[:, 0:32, :].reshape(128, 256), a1)
    for band in range(3):
        xa[band, :, 0:32, :] = own[:, 128 * band : 128 * band + 128].reshape(4, 32, 128)
    rows_copy.wait_recv()
    beyond = product(raw[:, 32:56, :].reshape(96, 256), a1)
    for band in range(3):
        xa[band, :, 32:56, :] = beyond[:, 128 * band : 128 * band + 128].reshape(4, 24, 128)

    deep = []
    for z in range(4):
        taps = [xa[2, z, pl.ds(i, 8, stride=4), :] for i in range(22)]
        deep.append((weighted(DEEP_LOW, taps), weighted(DEEP_HIGH, taps)))

    def partial(sz, sy, offset):
        filter_taps = (DEEP_LOW, DEEP_HIGH)[sz]
        planes = [z for z in range(4) if z + 8 - 4 * offset < 22]
        return weighted(
            [filter_taps[z + 8 - 4 * offset] for z in planes], [deep[z][sy] for z in planes]
        )

    offsets = (2, -2, -3, 1, -1)
    for index, offset in enumerate(offsets):
        for sz in range(2):
            for sy in range(2):
                part_out[index, sz, sy] = partial(sz, sy, offset)

    @pl.when(gy == 0)
    def _():
        pl.semaphore_wait(barrier, 16)
        signal(link, other_core)

    @pl.when(gy == 1)
    def _():
        pl.semaphore_wait(link, 1)

    part_copies = send_all(
        part_in,
        *(
            (part_out.at[index], part_in.at[index], along(offset))
            for index, offset in enumerate(offsets)
        ),
    )

    for z in range(4):
        for sx in range(2):
            taps = [xa[sx, z, pl.ds(j, 16, stride=2), :] for j in range(8)]
            zw[6 + z, sx] = weighted(LOWPASS, taps)
            zw[6 + z, 2 + sx] = weighted(HIGHPASS, taps)
    plane_copies = send_all(
        zw.at[0:6],
        (zw.at[6:10, 0:3], zw.at[2:6, 0:3], along(1)),
        (zw.at[6:8, 0:3], zw.at[10:12, 0:3], along(-1)),
        (zw.at[6:10, 3], zw.at[10:14, 3], along(-1)),
        (zw.at[8:10, 3], zw.at[4:6, 3], along(1)),
    )

    @pl.when(gy == 0)
    def _():
        signal(near_x, across_x(1, gy), across_x(-1, gy))

    @pl.when(gy == 0)
    def _():
        pl.semaphore_wait(near_x, 2)
        signal(mid_x, across_x(2, gy), across_x(-2, gy))

    lane = lax.broadcasted_iota(jnp.int32, (8, 128), 1)
    first_half = lane < 64
    zero = jnp.zeros((8, 128), jnp.float32)
    loads[2].wait()
    limits = [thr[t] for t in range(4)]
    squares = [limit * limit for limit in limits]

    part_copies.wait_recv()
    residual = [zero] * 4
    weight = [zero] * 4
    for sz in range(2):
        for sy in range(2):
            c = partial(sz, sy, 0)
            for index in range(5):
                c = c + part_in[index, sz, sy]
            cb[3, sz, sy, 8:16, :] = c
    coeff_copies = send_all(
        cb.at[0:5, :, :, 8:16, :],
        *(
            (cb.at[3, :, :, 8:16, :], cb.at[3 - offset, :, :, 8:16, :], along(offset))
            for offset in (3, -2, 2, -1, 1)
        ),
    )
    for sz in range(2):
        for sy in range(2):
            c = cb[3, sz, sy, 8:16, :]
            square = c * c
            for t in range(4):
                cut = jnp.clip(c, -limits[t], limits[t])
                kept = squares[t] / (squares[t] + square)
                cut = cut * cut
                if sz == 0 and sy == 0:
                    cut = jnp.where(first_half, zero, cut)
                    kept = jnp.where(first_half, zero, kept)
                residual[t] = residual[t] + cut
                weight[t] = weight[t] + kept

    def level_one(k, band):
        planes = [zw[2 * k + j, band] for j in range(8)]
        if band:
            db[k, 2 * band - 1, 8:24, :] = weighted(LOWPASS, planes)
        db[k, 2 * band, 8:24, :] = weighted(HIGHPASS, planes)

    @pl.when(gy == 0)
    def _():
        pl.semaphore_wait(mid_x, 2)
        signal(link, other_core)
        signal(near_z, across_z(3), across_z(-3))

    plane_copies.wait_recv()
    for k in range(2):
        for band in range(3):
            level_one(1 + k, band)
        level_one(2 + k, 3)

    def add_bands(first):
        def add_band(band, sums):
            sums = list(sums)
            for k in range(2):
                for half in range(2):
                    c = db[first + k, band, 8 + 8 * half : 16 + 8 * half, :]
                    square = c * c
                    for t in range(4):
                        cut = jnp.clip(c, -limits[t], limits[t])
                        sums[t] = sums[t] + cut * cut
                        sums[4 + t] = sums[4 + t] + squares[t] / (squares[t] + square)
            return tuple(sums)

        return add_band

    sums = lax.fori_loop(0, 5, add_bands(1), tuple(residual + weight))
    sums = lax.fori_loop(5, 7, add_bands(2), sums)

    line = jnp.zeros((1, 128), jnp.float32)
    for index, part in enumerate(sums):
        value = jnp.sum(jnp.sum(part, axis=0, keepdims=True), axis=1, keepdims=True)
        line = jnp.where(lane[0:1] == index, value, line)
    row[...] = line
    slot = gy * nx + gx
    arx[pl.ds(slot, 1)] = row[...].reshape(1, 1, 128)

    @pl.when(gy == 1)
    def _():
        pl.semaphore_wait(link, 1)

    x_copies = send_all(
        arx.at[0 : 2 * nx - 1],
        *(
            (row, arx.at[slot], across_x(offset, place))
            for offset in sorted(range(nx), key=lambda o: -min(o, nx - o))
            for place in (gy, other)
            if not (place is gy and offset == 0)
        ),
    )

    detail_copies = send_all(
        db.at[0:3, :, 8:24, :],
        (db.at[1:3, 0:5, 8:24, :], db.at[3:5, 0:5, 8:24, :], along(-1)),
        (db.at[2, 0:5, 8:24, :], db.at[0, 0:5, 8:24, :], along(1)),
        (db.at[2:4, 5:7, 8:24, :], db.at[0:2, 5:7, 8:24, :], along(1)),
        (db.at[2, 5:7, 8:24, :], db.at[4, 5:7, 8:24, :], along(-1)),
    )

    @pl.when(gy == 0)
    def _():
        pl.semaphore_wait(near_z, 2)
        signal(mid_z, across_z(2), across_z(-2))

    @pl.when(gy == 0)
    def _():
        pl.semaphore_wait(mid_z, 2)
        signal(link, other_core)

    x_copies.wait_recv()

    @pl.when(gy == 1)
    def _():
        pl.semaphore_wait(link, 1)

    tot[...] = jnp.sum(arx[...], axis=0)
    arz[pl.ds(gz, 1)] = tot[...].reshape(1, 1, 128)
    z_copies = send_all(
        arz.at[0 : nz - 1],
        *(
            (tot, arz.at[gz], across_z(offset))
            for offset in sorted(range(1, nz), key=lambda o: min(o, nz - o))
        ),
    )

    coeff_copies.wait_recv()
    deep_rows = send_all(
        cb.at[:, :, :, 8:16, :],
        (cb.at[:, :, :, 8:16, :], cb.at[:, :, :, 0:8, :], other_core),
    )

    detail_copies.wait_recv()
    detail_rows = send_all(
        db.at[:, :, 16:24, :], (db.at[:, :, 16:24, :], db.at[:, :, 0:8, :], other_core)
    )

    deep_rows.wait_recv()

    def deep_along_z(t, carry):
        limit = thr[t]
        for sy in range(2):
            for part in range(2):
                bands = []
                for sz in range(2):
                    values = []
                    for m in range(6):
                        c = cb[m, sz, sy, 8 * part : 8 * part + 8, :]
                        s = shrunk(c, limit)
                        values.append(jnp.where(first_half, c, s) if sz + sy == 0 else s)
                    bands.append(values)
                for k in range(5):
                    p = 3 + (k + 1) // 2
                    odd = (k + 1) % 2
                    order = [p - i for i in range(4)]
                    zs2[t, k, sy, 8 + 8 * part : 16 + 8 * part, :] = synthesis_pair(
                        [bands[0][i] for i in order], [bands[1][i] for i in order], odd
                    )
        return carry

    lax.fori_loop(0, 4, deep_along_z, 0)

    def deep_along_y(t, carry):
        for k in range(5):
            low = [zs2[t, k, 0, 8 - i : 24 - i, :] for i in range(4)]
            high = [zs2[t, k, 1, 8 - i : 24 - i, :] for i in range(4)]
            co[t, k, pl.ds(0, 16, stride=2), :] = synthesis_pair(low, high, 0)
            co[t, k, pl.ds(1, 16, stride=2), :] = synthesis_pair(low, high, 1)
        return carry

    lax.fori_loop(0, 4, deep_along_y, 0)
    loads[3].wait()
    cr[...] = product(co[:, :, 8:32, :].reshape(480, 128), a2t).reshape(4, 5, 24, 128)

    detail_rows.wait_recv()

    def along_z(t, carry):
        limit = thr[t]
        for part in range(3):
            rows = slice(8 * part, 8 * part + 8)

            def cut(band):
                return [shrunk(db[k, band, rows, :], limit) for k in range(5)]

            pairs = ((None, cut(0)), (cut(1), cut(2)), (cut(3), cut(4)), (cut(5), cut(6)))
            for band, (low, high) in enumerate(pairs):
                for e in range(2):
                    order = [3 + e - i for i in range(4)]
                    for odd in range(2):
                        value = weighted(HIGHPASS[odd::2], [high[i] for i in order])
                        if low is not None:
                            value = value + weighted(LOWPASS[odd::2], [low[i] for i in order])
                        zs1[2 * e + odd, t, band, rows, :] = value
        return carry

    lax.fori_loop(0, 4, along_z, 0)

    def along_y(t, carry):
        for part in range(3):
            rows = slice(8 * part, 8 * part + 8)
            low = [cr[t, k, rows, :] for k in range(5)]
            for e in range(2):
                order = [3 + e - i for i in range(4)]
                for odd in range(2):
                    zs1[2 * e + odd, t, 0, rows, :] = zs1[
                        2 * e + odd, t, 0, rows, :
                    ] + weighted(LOWPASS[odd::2], [low[i] for i in order])
        for z in range(4):
            for sx in range(2):
                low = [zs1[z, t, sx, 8 - i : 24 - i, :] for i in range(4)]
                high = [zs1[z, t, 2 + sx, 8 - i : 24 - i, :] for i in range(4)]
                fo[sx, z, t, pl.ds(0, 16, stride=2), :] = synthesis_pair(low, high, 0)
                fo[sx, z, t, pl.ds(1, 16, stride=2), :] = synthesis_pair(low, high, 1)
        return carry

    lax.fori_loop(0, 4, along_y, 0)
    loads[4].wait()
    both = jnp.concatenate([fo[0].reshape(512, 128), fo[1].reshape(512, 128)], axis=1)
    den[...] = product(both, a1t).reshape(4, 4, 32, 256)

    z_copies.wait_recv()
    full = jnp.sum(arz[...], axis=0)
    cells = float(4 * 32 * 256 * total * 2)
    weights = full[:, 4:8]
    gcv[...] = cells * full[:, 0:4] / (weights * weights)
    for group in groups:
        group.wait_send()


def solution(mesh):
    nx, nz = 8, 16
    return on_grid(mesh, nx, nz)


def on_grid(mesh, nx, nz):
    split = Mesh(
        mesh.devices.reshape(mesh.shape["cube"], nx, nz, mesh.shape["gy"]),
        ("cube", "gz_0", "gz_1", "gy"),
    )
    first = analysis_matrix(256)
    second = analysis_matrix(128)
    forward = np.concatenate([first, first[:, 0:128] @ second], axis=1)
    matrices = [in_two_parts(m) for m in (forward, first.T, second.T)]
    f32 = jnp.float32

    def body(noisy_cube, thresholds):
        den, gcv = pl.pallas_call(
            functools.partial(kernel, nx, nz),
            out_shape=(
                jax.ShapeDtypeStruct((4, 4, 32, 256), f32),
                jax.ShapeDtypeStruct((1, 4), f32),
            ),
            in_specs=[pl.BlockSpec(memory_space=pltpu.HBM)] * 5,
            out_specs=(
                pl.BlockSpec(memory_space=pltpu.VMEM),
                pl.BlockSpec(memory_space=pltpu.VMEM),
            ),
            scratch_shapes=[
                pltpu.SMEM((4,), f32),
                pltpu.VMEM((4, 56, 256), f32),
                pltpu.VMEM((3, 4, 56, 128), f32),
                pltpu.VMEM((16, 4, 16, 128), f32),
                pltpu.VMEM((5, 2, 2, 8, 128), f32),
                pltpu.VMEM((5, 2, 2, 8, 128), f32),
                pltpu.VMEM((5, 7, 24, 128), f32),
                pltpu.VMEM((6, 2, 2, 16, 128), f32),
                pltpu.VMEM((4, 5, 2, 24, 128), f32),
                pltpu.VMEM((4, 5, 32, 128), f32),
                pltpu.VMEM((4, 5, 24, 128), f32),
                pltpu.VMEM((4, 4, 4, 24, 128), f32),
                pltpu.VMEM((2, 4, 4, 32, 128), f32),
                pltpu.VMEM((2, 256, 384), jnp.bfloat16),
                pltpu.VMEM((2, 256, 256), jnp.bfloat16),
                pltpu.VMEM((2, 128, 128), jnp.bfloat16),
                pltpu.VMEM((1, 128), f32),
                pltpu.VMEM((1, 128), f32),
                pltpu.VMEM((2 * nx, 1, 128), f32),
                pltpu.VMEM((nz, 1, 128), f32),
                pltpu.SemaphoreType.DMA((5,)),
                pltpu.SemaphoreType.DMA((9,)),
                pltpu.SemaphoreType.DMA((9,)),
                pltpu.SemaphoreType.REGULAR,
                pltpu.SemaphoreType.REGULAR,
                pltpu.SemaphoreType.REGULAR,
                pltpu.SemaphoreType.REGULAR,
                pltpu.SemaphoreType.REGULAR,
            ],
            compiler_params=pltpu.CompilerParams(
                collective_id=0, has_side_effects=True, vmem_limit_bytes=12 * 1024 * 1024
            ),
        )(*(pltpu.with_memory_space_constraint(v, pltpu.HBM) for v in (thresholds, noisy_cube, *(jnp.asarray(m) for m in matrices))))
        return den, gcv.reshape(4)

    return jax.shard_map(
        body,
        mesh=split,
        in_specs=(P(CUBE_GZ, "gy", None), P()),
        out_specs=(P(CUBE_GZ, None, "gy", None), P("cube")),
        check_vma=False,
    )
```

```python
import functools

import jax
import jax.numpy as jnp
import numpy as np
from jax import lax
from jax.experimental import pallas as pl
from jax.experimental.pallas import tpu as pltpu
from jax.sharding import Mesh
from jax.sharding import PartitionSpec as P

MESH = pl.DeviceIdType.MESH
CUBE_GZ = ("cube", "gz_0", "gz_1")

LOWPASS = (
    0.2303778133088964,
    0.7148465705529155,
    0.6308807679298587,
    -0.0279837694168599,
    -0.1870348117190931,
    0.0308413818355607,
    0.0328830116668852,
    -0.010597401785069,
)
HIGHPASS = tuple(((-1) ** tap * LOWPASS[7 - tap] for tap in range(8)))


def composed(second):
    taps = np.zeros(22)
    for outer in range(8):
        for inner in range(8):
            taps[2 * outer + inner] += second[outer] * LOWPASS[inner]
    return tuple(float(tap) for tap in taps)


DEEP_LOW = composed(LOWPASS)
DEEP_HIGH = composed(HIGHPASS)


def analysis_matrix(length):
    matrix = np.zeros((length, length))
    for k in range(length // 2):
        for tap in range(8):
            matrix[(2 * k + tap) % length, k] += LOWPASS[tap]
            matrix[(2 * k + tap) % length, length // 2 + k] += HIGHPASS[tap]
    return matrix


def in_two_parts(matrix):
    exact = matrix.astype(np.float32)
    upper = exact.astype(jnp.bfloat16)
    lower = (exact - upper.astype(np.float32)).astype(jnp.bfloat16)
    return np.stack([upper, lower])


def product(values, parts):
    upper = values.astype(jnp.bfloat16)
    lower = (values - upper.astype(jnp.float32)).astype(jnp.bfloat16)
    dot = functools.partial(jnp.dot, preferred_element_type=jnp.float32)
    return dot(upper, parts[0]) + (dot(lower, parts[0]) + dot(upper, parts[1]))


def weighted(taps, values):
    result = taps[0] * values[0]
    for tap, value in zip(taps[1:], values[1:]):
        result = result + tap * value
    return result


def synthesis_pair(low, high, odd):
    return weighted(LOWPASS[odd::2], low) + weighted(HIGHPASS[odd::2], high)


def shrunk(values, limit):
    return values - jnp.clip(values, -limit, limit)


def kernel(
    nx,
    nz,
    thr_hbm,
    x_hbm,
    a1_hbm,
    a1t_hbm,
    a2t_hbm,
    den,
    gcv,
    thr,
    raw,
    xa,
    zw,
    part_out,
    part_in,
    db,
    cb,
    zs2,
    co,
    cr,
    zs1,
    fo,
    a1,
    a1t,
    a2t,
    row,
    tot,
    arx,
    arz,
    local_sem,
    send_sem,
    recv_sem,
    link,
    near_x,
    mid_x,
    near_z,
    mid_z,
):
    cube, gx, gz, gy = (lax.axis_index(n) for n in ("cube", "gz_0", "gz_1", "gy"))
    total = nx * nz
    flat = gx * nz + gz
    other = 1 - gy
    other_core = (cube, gx, gz, other)

    def along(offset, core=None):
        place = lax.rem(flat + (offset + total), total)
        return (cube, lax.div(place, nz), lax.rem(place, nz), gy if core is None else core)

    def across_x(offset, core):
        return (cube, lax.rem(gx + (offset + nx), nx), gz, core)

    def across_z(offset):
        return (cube, gx, lax.rem(gz + (offset + 2 * nz), nz), gy)

    groups = []

    def send_all(whole, *copies):
        index = len(groups)
        sems = (send_sem.at[index], recv_sem.at[index])
        for src, dst, device in copies:
            pltpu.make_async_remote_copy(
                src_ref=src,
                dst_ref=dst,
                send_sem=sems[0],
                recv_sem=sems[1],
                device_id=device,
                device_id_type=MESH,
            ).start()
        group = pltpu.make_async_remote_copy(
            src_ref=whole,
            dst_ref=whole,
            send_sem=sems[0],
            recv_sem=sems[1],
            device_id=other_core,
            device_id_type=MESH,
        )
        groups.append(group)
        return group

    def signal(sem, *devices):
        for device in devices:
            pl.semaphore_signal(sem, inc=1, device_id=device, device_id_type=MESH)

    loads = [pltpu.make_async_copy(x_hbm, raw.at[:, 0:32, :], local_sem.at[0])]
    for index, (src, dst) in enumerate(
        ((a1_hbm, a1), (thr_hbm, thr), (a2t_hbm, a2t), (a1t_hbm, a1t))
    ):
        loads.append(pltpu.make_async_copy(src, dst, local_sem.at[index + 1]))
    for load in loads:
        load.start()

    barrier = pltpu.get_barrier_semaphore()

    @pl.when(gy == 0)
    def _():
        signal(barrier, other_core)

    around = [along(offset, 0) for offset in (3, -3, 2, -2, 1, -1)]
    signal(barrier, *around, across_x(1, 0), across_x(-1, 0))

    @pl.when(gy == 1)
    def _():
        pl.semaphore_wait(barrier, 1)
        signal(link, other_core)

    @pl.when(gy == 0)
    def _():
        pl.semaphore_wait(link, 1)

    loads[0].wait()
    rows_copy = send_all(
        raw.at[:, 0:24, :], (raw.at[:, 0:24, :], raw.at[:, 32:56, :], other_core)
    )

    loads[1].wait()
    own = product(raw[:, 0:32, :].reshape(128, 256), a1)
    for band in range(3):
        xa[band, :, 0:32, :] = own[:, 128 * band : 128 * band + 128].reshape(4, 32, 128)
    rows_copy.wait_recv()
    beyond = product(raw[:, 32:56, :].reshape(96, 256), a1)
    for band in range(3):
        xa[band, :, 32:56, :] = beyond[:, 128 * band : 128 * band + 128].reshape(4, 24, 128)

    deep = []
    for z in range(4):
        taps = [xa[2, z, pl.ds(i, 8, stride=4), :] for i in range(22)]
        deep.append((weighted(DEEP_LOW, taps), weighted(DEEP_HIGH, taps)))

    def partial(sz, sy, offset):
        filter_taps = (DEEP_LOW, DEEP_HIGH)[sz]
        planes = [z for z in range(4) if z + 8 - 4 * offset < 22]
        return weighted(
            [filter_taps[z + 8 - 4 * offset] for z in planes], [deep[z][sy] for z in planes]
        )

    offsets = (2, -2, -3, 1, -1)
    for index, offset in enumerate(offsets):
        for sz in range(2):
            for sy in range(2):
                part_out[index, sz, sy] = partial(sz, sy, offset)

    @pl.when(gy == 0)
    def _():
        pl.semaphore_wait(barrier, 16)
        signal(link, other_core)

    @pl.when(gy == 1)
    def _():
        pl.semaphore_wait(link, 1)

    part_copies = send_all(
        part_in,
        *(
            (part_out.at[index], part_in.at[index], along(offset))
            for index, offset in enumerate(offsets)
        ),
    )

    for z in range(4):
        for sx in range(2):
            taps = [xa[sx, z, pl.ds(j, 16, stride=2), :] for j in range(8)]
            zw[6 + z, sx] = weighted(LOWPASS, taps)
            zw[6 + z, 2 + sx] = weighted(HIGHPASS, taps)
    plane_copies = send_all(
        zw.at[0:6],
        (zw.at[6:10], zw.at[2:6], along(1)),
        (zw.at[6:8], zw.at[10:12], along(-1)),
    )

    @pl.when(gy == 0)
    def _():
        signal(near_x, across_x(1, gy), across_x(-1, gy))

    @pl.when(gy == 0)
    def _():
        pl.semaphore_wait(near_x, 2)
        signal(mid_x, across_x(2, gy), across_x(-2, gy))

    lane = lax.broadcasted_iota(jnp.int32, (8, 128), 1)
    first_half = lane < 64
    zero = jnp.zeros((8, 128), jnp.float32)
    loads[2].wait()
    limits = [thr[t] for t in range(4)]
    squares = [limit * limit for limit in limits]

    part_copies.wait_recv()
    residual = [zero] * 4
    weight = [zero] * 4
    for sz in range(2):
        for sy in range(2):
            c = partial(sz, sy, 0)
            for index in range(5):
                c = c + part_in[index, sz, sy]
            cb[3, sz, sy, 8:16, :] = c
    coeff_copies = send_all(
        cb.at[0:5, :, :, 8:16, :],
        *(
            (cb.at[3, :, :, 8:16, :], cb.at[3 - offset, :, :, 8:16, :], along(offset))
            for offset in (3, -2, 2, -1, 1)
        ),
    )
    for sz in range(2):
        for sy in range(2):
            c = cb[3, sz, sy, 8:16, :]
            square = c * c
            for t in range(4):
                cut = jnp.clip(c, -limits[t], limits[t])
                kept = squares[t] / (squares[t] + square)
                cut = cut * cut
                if sz == 0 and sy == 0:
                    cut = jnp.where(first_half, zero, cut)
                    kept = jnp.where(first_half, zero, kept)
                residual[t] = residual[t] + cut
                weight[t] = weight[t] + kept

    def level_one(k, band):
        planes = [zw[2 * k + j, band] for j in range(8)]
        if band:
            db[k, 2 * band - 1, 8:24, :] = weighted(LOWPASS, planes)
        db[k, 2 * band, 8:24, :] = weighted(HIGHPASS, planes)

    @pl.when(gy == 0)
    def _():
        pl.semaphore_wait(mid_x, 2)
        signal(link, other_core)
        signal(near_z, across_z(3), across_z(-3))

    plane_copies.wait_recv()
    for k in range(2):
        for band in range(4):
            level_one(1 + k, band)

    def add_band(band, sums):
        sums = list(sums)
        for k in range(2):
            for half in range(2):
                c = db[1 + k, band, 8 + 8 * half : 16 + 8 * half, :]
                square = c * c
                for t in range(4):
                    cut = jnp.clip(c, -limits[t], limits[t])
                    sums[t] = sums[t] + cut * cut
                    sums[4 + t] = sums[4 + t] + squares[t] / (squares[t] + square)
        return tuple(sums)

    sums = lax.fori_loop(0, 7, add_band, tuple(residual + weight))

    line = jnp.zeros((1, 128), jnp.float32)
    for index, part in enumerate(sums):
        value = jnp.sum(jnp.sum(part, axis=0, keepdims=True), axis=1, keepdims=True)
        line = jnp.where(lane[0:1] == index, value, line)
    row[...] = line
    slot = gy * nx + gx
    arx[pl.ds(slot, 1)] = row[...].reshape(1, 1, 128)

    @pl.when(gy == 1)
    def _():
        pl.semaphore_wait(link, 1)

    x_copies = send_all(
        arx.at[0 : 2 * nx - 1],
        *(
            (row, arx.at[slot], across_x(offset, place))
            for offset in sorted(range(nx), key=lambda o: -min(o, nx - o))
            for place in (gy, other)
            if not (place is gy and offset == 0)
        ),
    )

    detail_copies = send_all(
        db.at[0:3, :, 8:24, :],
        (db.at[1:3, :, 8:24, :], db.at[3:5, :, 8:24, :], along(-1)),
        (db.at[2, :, 8:24, :], db.at[0, :, 8:24, :], along(1)),
    )

    @pl.when(gy == 0)
    def _():
        pl.semaphore_wait(near_z, 2)
        signal(mid_z, across_z(2), across_z(-2))

    @pl.when(gy == 0)
    def _():
        pl.semaphore_wait(mid_z, 2)
        signal(link, other_core)

    x_copies.wait_recv()

    @pl.when(gy == 1)
    def _():
        pl.semaphore_wait(link, 1)

    tot[...] = jnp.sum(arx[...], axis=0)
    arz[pl.ds(gz, 1)] = tot[...].reshape(1, 1, 128)
    z_copies = send_all(
        arz.at[0 : nz - 1],
        *(
            (tot, arz.at[gz], across_z(offset))
            for offset in sorted(range(1, nz), key=lambda o: min(o, nz - o))
        ),
    )

    coeff_copies.wait_recv()
    deep_rows = send_all(
        cb.at[:, :, :, 8:16, :],
        (cb.at[:, :, :, 8:16, :], cb.at[:, :, :, 0:8, :], other_core),
    )

    detail_copies.wait_recv()
    detail_rows = send_all(
        db.at[:, :, 16:24, :], (db.at[:, :, 16:24, :], db.at[:, :, 0:8, :], other_core)
    )

    deep_rows.wait_recv()

    def deep_along_z(t, carry):
        limit = thr[t]
        for sy in range(2):
            for part in range(2):
                bands = []
                for sz in range(2):
                    values = []
                    for m in range(6):
                        c = cb[m, sz, sy, 8 * part : 8 * part + 8, :]
                        s = shrunk(c, limit)
                        values.append(jnp.where(first_half, c, s) if sz + sy == 0 else s)
                    bands.append(values)
                for k in range(5):
                    p = 3 + (k + 1) // 2
                    odd = (k + 1) % 2
                    order = [p - i for i in range(4)]
                    zs2[t, k, sy, 8 + 8 * part : 16 + 8 * part, :] = synthesis_pair(
                        [bands[0][i] for i in order], [bands[1][i] for i in order], odd
                    )
        return carry

    lax.fori_loop(0, 4, deep_along_z, 0)

    def deep_along_y(t, carry):
        for k in range(5):
            low = [zs2[t, k, 0, 8 - i : 24 - i, :] for i in range(4)]
            high = [zs2[t, k, 1, 8 - i : 24 - i, :] for i in range(4)]
            co[t, k, pl.ds(0, 16, stride=2), :] = synthesis_pair(low, high, 0)
            co[t, k, pl.ds(1, 16, stride=2), :] = synthesis_pair(low, high, 1)
        return carry

    lax.fori_loop(0, 4, deep_along_y, 0)
    loads[3].wait()
    cr[...] = product(co[:, :, 8:32, :].reshape(480, 128), a2t).reshape(4, 5, 24, 128)

    detail_rows.wait_recv()

    def along_z(t, carry):
        limit = thr[t]
        for part in range(3):
            rows = slice(8 * part, 8 * part + 8)

            def cut(band):
                return [shrunk(db[k, band, rows, :], limit) for k in range(5)]

            pairs = ((None, cut(0)), (cut(1), cut(2)), (cut(3), cut(4)), (cut(5), cut(6)))
            for band, (low, high) in enumerate(pairs):
                for e in range(2):
                    order = [3 + e - i for i in range(4)]
                    for odd in range(2):
                        value = weighted(HIGHPASS[odd::2], [high[i] for i in order])
                        if low is not None:
                            value = value + weighted(LOWPASS[odd::2], [low[i] for i in order])
                        zs1[2 * e + odd, t, band, rows, :] = value
        return carry

    lax.fori_loop(0, 4, along_z, 0)

    def along_y(t, carry):
        for part in range(3):
            rows = slice(8 * part, 8 * part + 8)
            low = [cr[t, k, rows, :] for k in range(5)]
            for e in range(2):
                order = [3 + e - i for i in range(4)]
                for odd in range(2):
                    zs1[2 * e + odd, t, 0, rows, :] = zs1[
                        2 * e + odd, t, 0, rows, :
                    ] + weighted(LOWPASS[odd::2], [low[i] for i in order])
        for z in range(4):
            for sx in range(2):
                low = [zs1[z, t, sx, 8 - i : 24 - i, :] for i in range(4)]
                high = [zs1[z, t, 2 + sx, 8 - i : 24 - i, :] for i in range(4)]
                fo[sx, z, t, pl.ds(0, 16, stride=2), :] = synthesis_pair(low, high, 0)
                fo[sx, z, t, pl.ds(1, 16, stride=2), :] = synthesis_pair(low, high, 1)
        return carry

    lax.fori_loop(0, 4, along_y, 0)
    loads[4].wait()
    both = jnp.concatenate([fo[0].reshape(512, 128), fo[1].reshape(512, 128)], axis=1)
    den[...] = product(both, a1t).reshape(4, 4, 32, 256)

    z_copies.wait_recv()
    full = jnp.sum(arz[...], axis=0)
    cells = float(4 * 32 * 256 * total * 2)
    weights = full[:, 4:8]
    gcv[...] = cells * full[:, 0:4] / (weights * weights)
    for group in groups:
        group.wait_send()


def solution(mesh):
    nx, nz = 8, 16
    return on_grid(mesh, nx, nz)


def on_grid(mesh, nx, nz):
    split = Mesh(
        mesh.devices.reshape(mesh.shape["cube"], nx, nz, mesh.shape["gy"]),
        ("cube", "gz_0", "gz_1", "gy"),
    )
    first = analysis_matrix(256)
    second = analysis_matrix(128)
    forward = np.concatenate([first, first[:, 0:128] @ second], axis=1)
    matrices = [in_two_parts(m) for m in (forward, first.T, second.T)]
    f32 = jnp.float32

    def body(noisy_cube, thresholds):
        den, gcv = pl.pallas_call(
            functools.partial(kernel, nx, nz),
            out_shape=(
                jax.ShapeDtypeStruct((4, 4, 32, 256), f32),
                jax.ShapeDtypeStruct((1, 4), f32),
            ),
            in_specs=[pl.BlockSpec(memory_space=pltpu.HBM)] * 5,
            out_specs=(
                pl.BlockSpec(memory_space=pltpu.VMEM),
                pl.BlockSpec(memory_space=pltpu.VMEM),
            ),
            scratch_shapes=[
                pltpu.SMEM((4,), f32),
                pltpu.VMEM((4, 56, 256), f32),
                pltpu.VMEM((3, 4, 56, 128), f32),
                pltpu.VMEM((16, 4, 16, 128), f32),
                pltpu.VMEM((5, 2, 2, 8, 128), f32),
                pltpu.VMEM((5, 2, 2, 8, 128), f32),
                pltpu.VMEM((5, 7, 24, 128), f32),
                pltpu.VMEM((6, 2, 2, 16, 128), f32),
                pltpu.VMEM((4, 5, 2, 24, 128), f32),
                pltpu.VMEM((4, 5, 32, 128), f32),
                pltpu.VMEM((4, 5, 24, 128), f32),
                pltpu.VMEM((4, 4, 4, 24, 128), f32),
                pltpu.VMEM((2, 4, 4, 32, 128), f32),
                pltpu.VMEM((2, 256, 384), jnp.bfloat16),
                pltpu.VMEM((2, 256, 256), jnp.bfloat16),
                pltpu.VMEM((2, 128, 128), jnp.bfloat16),
                pltpu.VMEM((1, 128), f32),
                pltpu.VMEM((1, 128), f32),
                pltpu.VMEM((2 * nx, 1, 128), f32),
                pltpu.VMEM((nz, 1, 128), f32),
                pltpu.SemaphoreType.DMA((5,)),
                pltpu.SemaphoreType.DMA((9,)),
                pltpu.SemaphoreType.DMA((9,)),
                pltpu.SemaphoreType.REGULAR,
                pltpu.SemaphoreType.REGULAR,
                pltpu.SemaphoreType.REGULAR,
                pltpu.SemaphoreType.REGULAR,
                pltpu.SemaphoreType.REGULAR,
            ],
            compiler_params=pltpu.CompilerParams(
                collective_id=0, has_side_effects=True, vmem_limit_bytes=12 * 1024 * 1024
            ),
        )(*(pltpu.with_memory_space_constraint(v, pltpu.HBM) for v in (thresholds, noisy_cube, *(jnp.asarray(m) for m in matrices))))
        return den, gcv.reshape(4)

    return jax.shard_map(
        body,
        mesh=split,
        in_specs=(P(CUBE_GZ, "gy", None), P()),
        out_specs=(P(CUBE_GZ, None, "gy", None), P("cube")),
        check_vma=False,
    )
```

```python
import functools

import jax
import jax.numpy as jnp
import numpy as np
from jax import lax
from jax.experimental import pallas as pl
from jax.experimental.pallas import tpu as pltpu
from jax.sharding import Mesh
from jax.sharding import PartitionSpec as P

MESH = pl.DeviceIdType.MESH
CUBE_GZ = ("cube", "gz_0", "gz_1")

LOWPASS = (
    0.2303778133088964,
    0.7148465705529155,
    0.6308807679298587,
    -0.0279837694168599,
    -0.1870348117190931,
    0.0308413818355607,
    0.0328830116668852,
    -0.010597401785069,
)
HIGHPASS = tuple(((-1) ** tap * LOWPASS[7 - tap] for tap in range(8)))


def composed(second):
    taps = np.zeros(22)
    for outer in range(8):
        for inner in range(8):
            taps[2 * outer + inner] += second[outer] * LOWPASS[inner]
    return tuple(float(tap) for tap in taps)


DEEP_LOW = composed(LOWPASS)
DEEP_HIGH = composed(HIGHPASS)


def analysis_matrix(length):
    matrix = np.zeros((length, length))
    for k in range(length // 2):
        for tap in range(8):
            matrix[(2 * k + tap) % length, k] += LOWPASS[tap]
            matrix[(2 * k + tap) % length, length // 2 + k] += HIGHPASS[tap]
    return matrix


def in_two_parts(matrix):
    exact = matrix.astype(np.float32)
    upper = exact.astype(jnp.bfloat16)
    lower = (exact - upper.astype(np.float32)).astype(jnp.bfloat16)
    return np.stack([upper, lower])


def product(values, parts):
    upper = values.astype(jnp.bfloat16)
    lower = (values - upper.astype(jnp.float32)).astype(jnp.bfloat16)
    dot = functools.partial(jnp.dot, preferred_element_type=jnp.float32)
    return dot(upper, parts[0]) + (dot(lower, parts[0]) + dot(upper, parts[1]))


def weighted(taps, values):
    result = taps[0] * values[0]
    for tap, value in zip(taps[1:], values[1:]):
        result = result + tap * value
    return result


def synthesis_pair(low, high, odd):
    return weighted(LOWPASS[odd::2], low) + weighted(HIGHPASS[odd::2], high)


def shrunk(values, limit):
    return values - jnp.clip(values, -limit, limit)


def kernel(
    nx,
    nz,
    thr_hbm,
    x_hbm,
    a1_hbm,
    a1t_hbm,
    a2t_hbm,
    den,
    gcv,
    thr,
    raw,
    xa,
    zw,
    part_out,
    part_in,
    db,
    cb,
    zs2,
    co,
    cr,
    zs1,
    fo,
    a1,
    a1t,
    a2t,
    row,
    tot,
    arx,
    arz,
    local_sem,
    send_sem,
    recv_sem,
    link,
    near_x,
    mid_x,
    near_z,
    mid_z,
):
    cube, gx, gz, gy = (lax.axis_index(n) for n in ("cube", "gz_0", "gz_1", "gy"))
    total = nx * nz
    flat = gx * nz + gz
    other = 1 - gy
    other_core = (cube, gx, gz, other)

    def along(offset, core=None):
        place = lax.rem(flat + (offset + total), total)
        return (cube, lax.div(place, nz), lax.rem(place, nz), gy if core is None else core)

    def across_x(offset, core):
        return (cube, lax.rem(gx + (offset + nx), nx), gz, core)

    def across_z(offset):
        return (cube, gx, lax.rem(gz + (offset + 2 * nz), nz), gy)

    groups = []

    def send_all(whole, *copies):
        index = len(groups)
        sems = (send_sem.at[index], recv_sem.at[index])
        for src, dst, device in copies:
            pltpu.make_async_remote_copy(
                src_ref=src,
                dst_ref=dst,
                send_sem=sems[0],
                recv_sem=sems[1],
                device_id=device,
                device_id_type=MESH,
            ).start()
        group = pltpu.make_async_remote_copy(
            src_ref=whole,
            dst_ref=whole,
            send_sem=sems[0],
            recv_sem=sems[1],
            device_id=other_core,
            device_id_type=MESH,
        )
        groups.append(group)
        return group

    def signal(sem, *devices):
        for device in devices:
            pl.semaphore_signal(sem, inc=1, device_id=device, device_id_type=MESH)

    loads = [pltpu.make_async_copy(x_hbm, raw.at[:, 0:32, :], local_sem.at[0])]
    for index, (src, dst) in enumerate(
        ((a1_hbm, a1), (thr_hbm, thr), (a2t_hbm, a2t), (a1t_hbm, a1t))
    ):
        loads.append(pltpu.make_async_copy(src, dst, local_sem.at[index + 1]))
    for load in loads:
        load.start()

    barrier = pltpu.get_barrier_semaphore()

    @pl.when(gy == 0)
    def _():
        signal(barrier, other_core)

    around = [along(offset, 0) for offset in (3, -3, 2, -2, 1, -1)]
    signal(barrier, *around, across_x(1, 0), across_x(-1, 0))

    @pl.when(gy == 1)
    def _():
        pl.semaphore_wait(barrier, 1)
        signal(link, other_core)

    @pl.when(gy == 0)
    def _():
        pl.semaphore_wait(link, 1)

    loads[0].wait()
    rows_copy = send_all(
        raw.at[:, 0:24, :], (raw.at[:, 0:24, :], raw.at[:, 32:56, :], other_core)
    )

    loads[1].wait()
    own = product(raw[:, 0:32, :].reshape(128, 256), a1)
    for band in range(3):
        xa[band, :, 0:32, :] = own[:, 128 * band : 128 * band + 128].reshape(4, 32, 128)
    rows_copy.wait_recv()
    beyond = product(raw[:, 32:56, :].reshape(96, 256), a1)
    for band in range(3):
        xa[band, :, 32:56, :] = beyond[:, 128 * band : 128 * band + 128].reshape(4, 24, 128)

    deep = []
    for z in range(4):
        taps = [xa[2, z, pl.ds(i, 8, stride=4), :] for i in range(22)]
        deep.append((weighted(DEEP_LOW, taps), weighted(DEEP_HIGH, taps)))

    def partial(sz, sy, offset):
        filter_taps = (DEEP_LOW, DEEP_HIGH)[sz]
        planes = [z for z in range(4) if z + 8 - 4 * offset < 22]
        return weighted(
            [filter_taps[z + 8 - 4 * offset] for z in planes], [deep[z][sy] for z in planes]
        )

    offsets = (2, -2, -3, 1, -1)
    for index, offset in enumerate(offsets):
        for sz in range(2):
            for sy in range(2):
                part_out[index, sz, sy] = partial(sz, sy, offset)

    @pl.when(gy == 0)
    def _():
        pl.semaphore_wait(barrier, 16)
        signal(link, other_core)

    @pl.when(gy == 1)
    def _():
        pl.semaphore_wait(link, 1)

    part_copies = send_all(
        part_in,
        *(
            (part_out.at[index], part_in.at[index], along(offset))
            for index, offset in enumerate(offsets)
        ),
    )

    for z in range(4):
        for sx in range(2):
            taps = [xa[sx, z, pl.ds(j, 16, stride=2), :] for j in range(8)]
            zw[6 + z, sx] = weighted(LOWPASS, taps)
            zw[6 + z, 2 + sx] = weighted(HIGHPASS, taps)
    plane_copies = send_all(
        zw.at[0:6],
        (zw.at[6:10], zw.at[2:6], along(1)),
        (zw.at[6:8], zw.at[10:12], along(-1)),
    )

    @pl.when(gy == 0)
    def _():
        signal(near_x, across_x(1, gy), across_x(-1, gy))

    @pl.when(gy == 0)
    def _():
        pl.semaphore_wait(near_x, 2)
        signal(mid_x, across_x(2, gy), across_x(-2, gy))

    lane = lax.broadcasted_iota(jnp.int32, (8, 128), 1)
    first_half = lane < 64
    zero = jnp.zeros((8, 128), jnp.float32)
    loads[2].wait()
    limits = [thr[t] for t in range(4)]
    squares = [limit * limit for limit in limits]

    part_copies.wait_recv()
    residual = [zero] * 4
    weight = [zero] * 4
    for sz in range(2):
        for sy in range(2):
            c = partial(sz, sy, 0)
            for index in range(5):
                c = c + part_in[index, sz, sy]
            cb[3, sz, sy, 8:16, :] = c
    for sz in range(2):
        for sy in range(2):
            c = cb[3, sz, sy, 8:16, :]
            square = c * c
            for t in range(4):
                cut = jnp.clip(c, -limits[t], limits[t])
                kept = squares[t] / (squares[t] + square)
                cut = cut * cut
                if sz == 0 and sy == 0:
                    cut = jnp.where(first_half, zero, cut)
                    kept = jnp.where(first_half, zero, kept)
                residual[t] = residual[t] + cut
                weight[t] = weight[t] + kept

    def level_one(k, band):
        planes = [zw[2 * k + j, band] for j in range(8)]
        if band:
            db[k, 2 * band - 1, 8:24, :] = weighted(LOWPASS, planes)
        db[k, 2 * band, 8:24, :] = weighted(HIGHPASS, planes)

    @pl.when(gy == 0)
    def _():
        pl.semaphore_wait(mid_x, 2)
        signal(link, other_core)
        signal(near_z, across_z(3), across_z(-3))

    plane_copies.wait_recv()
    for k in range(2):
        for band in range(4):
            level_one(1 + k, band)

    def add_band(band, sums):
        sums = list(sums)
        for k in range(2):
            for half in range(2):
                c = db[1 + k, band, 8 + 8 * half : 16 + 8 * half, :]
                square = c * c
                for t in range(4):
                    cut = jnp.clip(c, -limits[t], limits[t])
                    sums[t] = sums[t] + cut * cut
                    sums[4 + t] = sums[4 + t] + squares[t] / (squares[t] + square)
        return tuple(sums)

    sums = lax.fori_loop(0, 7, add_band, tuple(residual + weight))

    line = jnp.zeros((1, 128), jnp.float32)
    for index, part in enumerate(sums):
        value = jnp.sum(jnp.sum(part, axis=0, keepdims=True), axis=1, keepdims=True)
        line = jnp.where(lane[0:1] == index, value, line)
    row[...] = line
    slot = gy * nx + gx
    arx[pl.ds(slot, 1)] = row[...].reshape(1, 1, 128)

    @pl.when(gy == 1)
    def _():
        pl.semaphore_wait(link, 1)

    x_copies = send_all(
        arx.at[0 : 2 * nx - 1],
        *(
            (row, arx.at[slot], across_x(offset, place))
            for offset in sorted(range(nx), key=lambda o: -min(o, nx - o))
            for place in (gy, other)
            if not (place is gy and offset == 0)
        ),
    )

    coeff_copies = send_all(
        cb.at[0:5, :, :, 8:16, :],
        *(
            (cb.at[3, :, :, 8:16, :], cb.at[3 - offset, :, :, 8:16, :], along(offset))
            for offset in (3, -2, 2, -1, 1)
        ),
    )
    detail_copies = send_all(
        db.at[0:3, :, 8:24, :],
        (db.at[1:3, :, 8:24, :], db.at[3:5, :, 8:24, :], along(-1)),
        (db.at[2, :, 8:24, :], db.at[0, :, 8:24, :], along(1)),
    )

    @pl.when(gy == 0)
    def _():
        pl.semaphore_wait(near_z, 2)
        signal(mid_z, across_z(2), across_z(-2))

    @pl.when(gy == 0)
    def _():
        pl.semaphore_wait(mid_z, 2)
        signal(link, other_core)

    x_copies.wait_recv()

    @pl.when(gy == 1)
    def _():
        pl.semaphore_wait(link, 1)

    tot[...] = jnp.sum(arx[...], axis=0)
    arz[pl.ds(gz, 1)] = tot[...].reshape(1, 1, 128)
    z_copies = send_all(
        arz.at[0 : nz - 1],
        *(
            (tot, arz.at[gz], across_z(offset))
            for offset in sorted(range(1, nz), key=lambda o: min(o, nz - o))
        ),
    )

    coeff_copies.wait_recv()
    deep_rows = send_all(
        cb.at[:, :, :, 8:16, :],
        (cb.at[:, :, :, 8:16, :], cb.at[:, :, :, 0:8, :], other_core),
    )

    detail_copies.wait_recv()
    detail_rows = send_all(
        db.at[:, :, 16:24, :], (db.at[:, :, 16:24, :], db.at[:, :, 0:8, :], other_core)
    )

    deep_rows.wait_recv()

    def deep_along_z(t, carry):
        limit = thr[t]
        for sy in range(2):
            for part in range(2):
                bands = []
                for sz in range(2):
                    values = []
                    for m in range(6):
                        c = cb[m, sz, sy, 8 * part : 8 * part + 8, :]
                        s = shrunk(c, limit)
                        values.append(jnp.where(first_half, c, s) if sz + sy == 0 else s)
                    bands.append(values)
                for k in range(5):
                    p = 3 + (k + 1) // 2
                    odd = (k + 1) % 2
                    order = [p - i for i in range(4)]
                    zs2[t, k, sy, 8 + 8 * part : 16 + 8 * part, :] = synthesis_pair(
                        [bands[0][i] for i in order], [bands[1][i] for i in order], odd
                    )
        return carry

    lax.fori_loop(0, 4, deep_along_z, 0)

    def deep_along_y(t, carry):
        for k in range(5):
            low = [zs2[t, k, 0, 8 - i : 24 - i, :] for i in range(4)]
            high = [zs2[t, k, 1, 8 - i : 24 - i, :] for i in range(4)]
            co[t, k, pl.ds(0, 16, stride=2), :] = synthesis_pair(low, high, 0)
            co[t, k, pl.ds(1, 16, stride=2), :] = synthesis_pair(low, high, 1)
        return carry

    lax.fori_loop(0, 4, deep_along_y, 0)
    loads[3].wait()
    cr[...] = product(co[:, :, 8:32, :].reshape(480, 128), a2t).reshape(4, 5, 24, 128)

    detail_rows.wait_recv()

    def along_z(t, carry):
        limit = thr[t]
        for part in range(3):
            rows = slice(8 * part, 8 * part + 8)

            def cut(band):
                return [shrunk(db[k, band, rows, :], limit) for k in range(5)]

            pairs = ((None, cut(0)), (cut(1), cut(2)), (cut(3), cut(4)), (cut(5), cut(6)))
            for band, (low, high) in enumerate(pairs):
                for e in range(2):
                    order = [3 + e - i for i in range(4)]
                    for odd in range(2):
                        value = weighted(HIGHPASS[odd::2], [high[i] for i in order])
                        if low is not None:
                            value = value + weighted(LOWPASS[odd::2], [low[i] for i in order])
                        zs1[2 * e + odd, t, band, rows, :] = value
        return carry

    lax.fori_loop(0, 4, along_z, 0)

    def along_y(t, carry):
        for part in range(3):
            rows = slice(8 * part, 8 * part + 8)
            low = [cr[t, k, rows, :] for k in range(5)]
            for e in range(2):
                order = [3 + e - i for i in range(4)]
                for odd in range(2):
                    zs1[2 * e + odd, t, 0, rows, :] = zs1[
                        2 * e + odd, t, 0, rows, :
                    ] + weighted(LOWPASS[odd::2], [low[i] for i in order])
        for z in range(4):
            for sx in range(2):
                low = [zs1[z, t, sx, 8 - i : 24 - i, :] for i in range(4)]
                high = [zs1[z, t, 2 + sx, 8 - i : 24 - i, :] for i in range(4)]
                fo[sx, z, t, pl.ds(0, 16, stride=2), :] = synthesis_pair(low, high, 0)
                fo[sx, z, t, pl.ds(1, 16, stride=2), :] = synthesis_pair(low, high, 1)
        return carry

    lax.fori_loop(0, 4, along_y, 0)
    loads[4].wait()
    both = jnp.concatenate([fo[0].reshape(512, 128), fo[1].reshape(512, 128)], axis=1)
    den[...] = product(both, a1t).reshape(4, 4, 32, 256)

    z_copies.wait_recv()
    full = jnp.sum(arz[...], axis=0)
    cells = float(4 * 32 * 256 * total * 2)
    weights = full[:, 4:8]
    gcv[...] = cells * full[:, 0:4] / (weights * weights)
    for group in groups:
        group.wait_send()


def solution(mesh):
    nx, nz = 8, 16
    return on_grid(mesh, nx, nz)


def on_grid(mesh, nx, nz):
    split = Mesh(
        mesh.devices.reshape(mesh.shape["cube"], nx, nz, mesh.shape["gy"]),
        ("cube", "gz_0", "gz_1", "gy"),
    )
    first = analysis_matrix(256)
    second = analysis_matrix(128)
    forward = np.concatenate([first, first[:, 0:128] @ second], axis=1)
    matrices = [in_two_parts(m) for m in (forward, first.T, second.T)]
    f32 = jnp.float32

    def body(noisy_cube, thresholds):
        den, gcv = pl.pallas_call(
            functools.partial(kernel, nx, nz),
            out_shape=(
                jax.ShapeDtypeStruct((4, 4, 32, 256), f32),
                jax.ShapeDtypeStruct((1, 4), f32),
            ),
            in_specs=[pl.BlockSpec(memory_space=pltpu.HBM)] * 5,
            out_specs=(
                pl.BlockSpec(memory_space=pltpu.VMEM),
                pl.BlockSpec(memory_space=pltpu.VMEM),
            ),
            scratch_shapes=[
                pltpu.SMEM((4,), f32),
                pltpu.VMEM((4, 56, 256), f32),
                pltpu.VMEM((3, 4, 56, 128), f32),
                pltpu.VMEM((16, 4, 16, 128), f32),
                pltpu.VMEM((5, 2, 2, 8, 128), f32),
                pltpu.VMEM((5, 2, 2, 8, 128), f32),
                pltpu.VMEM((5, 7, 24, 128), f32),
                pltpu.VMEM((6, 2, 2, 16, 128), f32),
                pltpu.VMEM((4, 5, 2, 24, 128), f32),
                pltpu.VMEM((4, 5, 32, 128), f32),
                pltpu.VMEM((4, 5, 24, 128), f32),
                pltpu.VMEM((4, 4, 4, 24, 128), f32),
                pltpu.VMEM((2, 4, 4, 32, 128), f32),
                pltpu.VMEM((2, 256, 384), jnp.bfloat16),
                pltpu.VMEM((2, 256, 256), jnp.bfloat16),
                pltpu.VMEM((2, 128, 128), jnp.bfloat16),
                pltpu.VMEM((1, 128), f32),
                pltpu.VMEM((1, 128), f32),
                pltpu.VMEM((2 * nx, 1, 128), f32),
                pltpu.VMEM((nz, 1, 128), f32),
                pltpu.SemaphoreType.DMA((5,)),
                pltpu.SemaphoreType.DMA((9,)),
                pltpu.SemaphoreType.DMA((9,)),
                pltpu.SemaphoreType.REGULAR,
                pltpu.SemaphoreType.REGULAR,
                pltpu.SemaphoreType.REGULAR,
                pltpu.SemaphoreType.REGULAR,
                pltpu.SemaphoreType.REGULAR,
            ],
            compiler_params=pltpu.CompilerParams(
                collective_id=0, has_side_effects=True, vmem_limit_bytes=12 * 1024 * 1024
            ),
        )(*(pltpu.with_memory_space_constraint(v, pltpu.HBM) for v in (thresholds, noisy_cube, *(jnp.asarray(m) for m in matrices))))
        return den, gcv.reshape(4)

    return jax.shard_map(
        body,
        mesh=split,
        in_specs=(P(CUBE_GZ, "gy", None), P()),
        out_specs=(P(CUBE_GZ, None, "gy", None), P("cube")),
        check_vma=False,
    )
```
